32 devices in a mesh: row: 2 (over y), col: 4 (over z), depth: 4 (over x, core).
Axes of the slice: x: 2, y: 2, z: 4, core: 2. Of those that a mesh axis runs over, the one named last changes fastest.
Arguments:
- state_matrix: float32 [6144, 6144], P('row', 'col'), as said below
- gram_factor: float32 [6144, 256], P(('col', 'depth'), 'row'), as said below
Outputs:
- squared: float32 [6144, 6144], P('row', ('col', 'depth'))
- appended: float32 [6144, 256], P(('row', 'col', 'depth'))
- norm_ratio: float32 [256], replicated
Inputs may be any that keep to these rules, and one draw needn't show every extreme that they name: `gram_factor`: entries whose scale grows up to about ninefold along the rows; the columns differ in scale by up to tenfold. `state_matrix`: A real matrix with entries of order one on the diagonal and smaller ones elsewhere.
All inputs are finite; a program needn't handle non-finite values.
Results may differ from the reference program's by a relative error of at most 0.000073.
Values sent between devices are 32-bit elements; how exact they have to be, the bound alone decides.
A program may use at most 128 MiB of HBM per device.

```python
import math
import jax
import jax.numpy as jnp
from jax import lax

ORDER = 6144
RANK = 256


def draw_state_matrix(key, part):
    first, second, third = jax.random.split(jax.random.fold_in(key, 11), 3)
    noise = jax.random.normal(first, (ORDER, ORDER), jnp.float32)
    magnitude = jax.random.uniform(second, (ORDER,), jnp.float32, 0.1, 0.9)
    signs = jnp.where(jax.random.uniform(third, (ORDER,), jnp.float32) < 0.5, -1.0, 1.0)
    return noise * (0.6 / math.sqrt(ORDER)) + jnp.diag(signs * magnitude)


def draw_gram_factor(key, part):
    first, second, third = jax.random.split(jax.random.fold_in(key, 23), 3)
    positions = jnp.arange(ORDER, dtype=jnp.float32) / ORDER
    row_scale = jnp.exp(math.log(3.0) * positions + jax.random.uniform(second, (ORDER,), jnp.float32, 0.0, math.log(3.0)))
    col_scale = jnp.exp(jax.random.uniform(third, (RANK,), jnp.float32, math.log(0.3), math.log(3.0)))
    noise = jax.random.normal(first, (ORDER, RANK), jnp.float32)
    return noise * row_scale[:, None] * col_scale[None, :]


def setup_inputs(seed: int = 0) -> dict:
    streams_of = jax.random.split(jax.random.key(seed), 3)
    state_matrix = draw_state_matrix(jax.random.fold_in(streams_of[2], 71), 0)
    gram_factor = draw_gram_factor(jax.random.fold_in(streams_of[2], 71), 0)
    return {"state_matrix": state_matrix, "gram_factor": gram_factor}


def reference(state_matrix, gram_factor):
    squared = jnp.dot(state_matrix, state_matrix, preferred_element_type=jnp.float32, precision=lax.Precision.HIGHEST)
    appended = jnp.dot(state_matrix, gram_factor, preferred_element_type=jnp.float32, precision=lax.Precision.HIGHEST)
    new_sq = lax.optimization_barrier(jnp.sum(appended * appended, axis=0))
    old_sq = lax.optimization_barrier(jnp.sum(gram_factor * gram_factor, axis=0))
    norm_ratio = jnp.sqrt(new_sq) / jnp.sqrt(old_sq + 1e-06)
    return (squared, appended, norm_ratio)
```

```python
import functools

import jax
import jax.numpy as jnp
from jax import lax
from jax.experimental import pallas as pl
from jax.experimental.pallas import tpu as pltpu
from jax.sharding import PartitionSpec as P


MESH = pl.DeviceIdType.MESH
VMEM_BYTES = 66_900_000


def split(value):
    high = value.astype(jnp.bfloat16)
    return high, (value - high.astype(jnp.float32)).astype(jnp.bfloat16)


def dot(left, right):
    return jnp.dot(left, right, preferred_element_type=jnp.float32)


def kernel(
    planes, a_hbm, z_hbm, sq_hbm, app_ref, norm_ref,
    left, left_hi, left_lo, far_rows, right_hi, right_lo, part, got_core, got_x,
    fac, fac_hi, fac_lo, terms, t_core, t_x, t_z, sums, s_got, s_z,
    own_sem, rows_sem, out_sem, fac_own_sem, z_send, z_recv, y_send, y_recv, core_send, core_recv,
    x_send, x_recv, small_send, small_recv, tz_send, tz_recv, sz_send, sz_recv,
):
    y, c, d = lax.axis_index("row"), lax.axis_index("col"), lax.axis_index("depth")
    x, k = lax.div(d, 2), lax.rem(d, 2)
    core_mate = {"depth": d + 1 - 2 * k}
    x_mate = {"depth": lax.rem(d + 2, 4)}
    y_mate = {"row": 1 - y}
    size = left_hi.shape[0]
    chunks = left.shape[1] // size
    per_row = a_hbm.shape[0] // a_hbm.shape[1]
    block = a_hbm.shape[1]
    inner = (c > 0) & (c < planes - 1)
    own_cols = pl.ds(pl.multiple_of(d * size, size), size)

    def rows(i):
        return pl.ds(pl.multiple_of(i * size, size), size)

    def remote(src, dst, send, recv, target):
        return pltpu.make_async_remote_copy(
            src_ref=src, dst_ref=dst, send_sem=send, recv_sem=recv, device_id=target, device_id_type=MESH
        )

    def hop(way, b, i, own=False):
        src = a_hbm.at[rows(i), own_cols] if own else left.at[b, rows(i)]
        target = {"col": c + 1 - 2 * way}
        return remote(src, left.at[b, rows(i)], z_send.at[way, b, i], z_recv.at[b, i], target)

    def has(way):
        return c < planes - 1 if way == 0 else c > 0

    def send_own(i):
        for way in (0, 1):
            @pl.when(has(way))
            def _():
                hop(way, c, i, own=True).start()

    def arrivals(i):
        for b in range(planes):
            @pl.when(b != c)
            def _():
                hop(0, b, i).wait_recv()

    def forward(i):
        for far in range(1, planes):
            for way in (0, 1):
                b = c - far if way == 0 else c + far
                @pl.when(has(way) & (b >= 0) & (b < planes))
                def _():
                    hop(way, b, i).wait_recv()
                    hop(way, b, i).start()

    def own_copy(i):
        return pltpu.make_async_copy(a_hbm.at[rows(i), own_cols], left.at[c, rows(i)], own_sem.at[i])

    def near_copy(q, j):
        src = a_hbm.at[pl.ds(pl.multiple_of(q * block + d * size, size), size), pl.ds(j * size, size)]
        return pltpu.make_async_copy(src, part.at[q, j // 2, j % 2], rows_sem.at[q, j])

    def y_copy(q, j):
        src = a_hbm.at[pl.ds(pl.multiple_of(q * block + d * size, size), size), pl.ds(j * size, size)]
        return remote(src, far_rows.at[q, j], y_send.at[q, j], y_recv.at[q, j], y_mate)

    half = z_hbm.shape[1]
    lanes = pl.ds(pl.multiple_of(y * half, half), half)
    fac_own = pltpu.make_async_copy(z_hbm, fac.at[:, lanes], fac_own_sem.at[0])
    fac_y = remote(z_hbm, fac.at[:, lanes], small_send.at[0], small_recv.at[0], y_mate)
    fac_y.start()
    fac_own.start()
    send_own(0)
    send_own(1)
    for q in range(per_row):
        for j in range(4):
            y_copy(q, j).start()
    for i in range(chunks):
        own_copy(i).start()
    @pl.when(jnp.logical_not(inner))
    def _():
        for i in range(2, chunks):
            send_own(i)
    for q in range(per_row):
        for j in range(4):
            near_copy(q, j).start()

    def keep_right(value, q, j, owner):
        high, low = split(value)
        at = pl.ds(pl.multiple_of((owner * per_row + q) * size, size), size)
        right_hi[j // 2, at, j % 2 * size : (j % 2 + 1) * size] = high
        right_lo[j // 2, at, j % 2 * size : (j % 2 + 1) * size] = low

    for i in range(chunks):
        own_copy(i).wait()
    fac_own.wait()
    fac_y.wait_recv()
    fac_hi[...], fac_lo[...] = split(fac[...])
    piece = terms.shape[3]

    def term(i, _):
        high, low = split(left[c, rows(i)])
        value = dot(high, fac_hi[...]) + dot(high, fac_lo[...]) + dot(low, fac_hi[...])
        for half_k in (0, 1):
            terms[lax.div(i, 2), lax.rem(i, 2), half_k] = value[half_k * piece : (half_k + 1) * piece]
        return 0

    lax.fori_loop(0, chunks, term, 0)
    for q in range(per_row):
        for j in range(4):
            near_copy(q, j).wait()
            keep_right(part[q, j // 2, j % 2], q, j, y)
    t_core_copy = remote(terms.at[:, :, 1 - k], t_core, small_send.at[1], small_recv.at[1], core_mate)
    t_core_copy.start()
    t_core_copy.wait_recv()
    for b in range(planes):
        t_core[b, 0] += terms[b, 0, k]
        t_core[b, 1] += terms[b, 1, k]
    @pl.when(inner)
    def _():
        forward(0)
        send_own(2)
    t_x_copy = remote(t_core.at[:, 1 - x], t_x, small_send.at[2], small_recv.at[2], x_mate)
    t_x_copy.start()
    t_x_copy.wait_recv()
    for b in range(planes):
        t_x[b] += t_core[b, x]
    @pl.when(inner)
    def _():
        forward(1)
        send_own(3)

    def tz_copy(far):
        b = lax.rem(c + far, planes)
        return remote(t_x.at[b], t_z.at[c], tz_send.at[far - 1], tz_recv.at[c], {"col": b})

    def tz_arrival(b):
        return remote(t_x.at[0], t_z.at[b], tz_send.at[0], tz_recv.at[b], {"col": b})

    for far in range(1, planes):
        tz_copy(far).start()
    ahead = 4
    @pl.when(inner)
    def _():
        for i in range(2, ahead):
            forward(i)
            send_own(i + 2)

    for j in range(4):
        for q in range(per_row):
            y_copy(q, j).wait_recv()
            keep_right(far_rows[q, j], q, j, 1 - y)

    def s_copy(stage, target):
        return remote(sums.at[stage], s_got.at[stage], small_send.at[3 + stage], small_recv.at[3 + stage], target)

    def sz_copy(far):
        b = lax.rem(c + far, planes)
        return remote(sums.at[3], s_z.at[c], sz_send.at[far - 1], sz_recv.at[c], {"col": b})

    def sz_arrival(b):
        return remote(sums.at[3], s_z.at[b], sz_send.at[0], sz_recv.at[b], {"col": b})

    def small(step):
        if step == 0:
            for b in range(planes):
                @pl.when(b != c)
                def _():
                    tz_arrival(b).wait_recv()
            t_z[c] = t_x[c]
            total = t_z[0]
            for b in range(1, planes):
                total = total + t_z[b]
            app_ref[...] = total
            new = jnp.sum(total * total, axis=0, keepdims=True)
            old = jnp.sum(fac[...] * fac[...], axis=0, keepdims=True) * 0.5
            sums[0, 0:1] = new
            sums[0, 1:2] = old
            s_copy(0, core_mate).start()
        elif step == 1:
            s_copy(0, core_mate).wait_recv()
            sums[1, 0:2] = sums[0, 0:2] + s_got[0, 0:2]
            s_copy(1, x_mate).start()
        elif step == 2:
            s_copy(1, x_mate).wait_recv()
            sums[2, 0:2] = sums[1, 0:2] + s_got[1, 0:2]
            s_copy(2, y_mate).start()
        elif step == 3:
            s_copy(2, y_mate).wait_recv()
            sums[3, 0:2] = sums[2, 0:2] + s_got[2, 0:2]
            for far in range(1, planes):
                sz_copy(far).start()
        elif step == 4:
            for b in range(planes):
                @pl.when(b != c)
                def _():
                    sz_arrival(b).wait_recv()
            s_z[c, 0:2] = sums[3, 0:2]
            both = s_z[0, 0:2]
            for b in range(1, planes):
                both = both + s_z[b, 0:2]
            norm_ref[...] = jnp.sqrt(both[0:1]) / jnp.sqrt(both[1:2] + 1e-06)

    def core_copy(i):
        return remote(
            part.at[lax.rem(i, 2), :, 1 - k], got_core.at[i], core_send.at[i], core_recv.at[i], core_mate
        )

    def x_copy(i):
        return remote(got_core.at[i, 1 - x], got_x.at[i], x_send.at[i], x_recv.at[i], x_mate)

    def out_copy(i):
        return pltpu.make_async_copy(got_x.at[i], sq_hbm.at[rows(i)], out_sem.at[i])

    def compute(i):
        for b in range(planes):
            high, low = split(left[b, rows(i)])
            left_hi[:, b * size : (b + 1) * size] = high
            left_lo[:, b * size : (b + 1) * size] = low

        def side(s, _):
            value = dot(left_hi[...], right_hi[s]) + dot(left_hi[...], right_lo[s]) + dot(left_lo[...], right_hi[s])
            part[lax.rem(i, 2), s, 0] = value[:, :size]
            part[lax.rem(i, 2), s, 1] = value[:, size:]
            return 0

        lax.fori_loop(0, 2, side, 0)

    def after_core(i):
        core_copy(i).wait_recv()
        got_core[i, 1 - x] += part[lax.rem(i, 2), 1 - x, k]
        got_core[i, x] += part[lax.rem(i, 2), x, k]
        x_copy(i).start()

    def after_x(i):
        x_copy(i).wait_recv()
        got_x[i] += got_core[i, x]
        out_copy(i).start()

    def step(i, _):
        @pl.when(inner & (i + ahead < chunks))
        def _():
            forward(i + ahead)
            @pl.when(i + ahead + 2 < chunks)
            def _():
                send_own(i + ahead + 2)
        @pl.when(jnp.logical_not(inner))
        def _():
            arrivals(i)
        @pl.when(i >= 2)
        def _():
            core_copy(i - 2).wait_send()
        compute(i)
        @pl.when(i >= 1)
        def _():
            after_core(i - 1)
        core_copy(i).start()
        @pl.when(i >= 2)
        def _():
            after_x(i - 2)
        for at in range(5):
            @pl.when(i == at + chunks - 5)
            def _():
                small(at)
        return 0

    lax.fori_loop(0, chunks, step, 0)
    after_core(chunks - 1)
    after_x(chunks - 2)
    after_x(chunks - 1)

    core_copy(chunks - 2).wait_send()
    core_copy(chunks - 1).wait_send()
    fac_y.wait_send()
    t_core_copy.wait_send()
    t_x_copy.wait_send()
    for far in range(1, planes):
        tz_copy(far).wait_send()
        sz_copy(far).wait_send()
    for stage, mate in enumerate((core_mate, x_mate, y_mate)):
        s_copy(stage, mate).wait_send()
    for q in range(per_row):
        for j in range(4):
            y_copy(q, j).wait_send()

    def finish(i, _):
        x_copy(i).wait_send()
        out_copy(i).wait()
        for b in range(planes):
            for way in (0, 1):
                sends = (b <= c) if way == 0 else (b >= c)
                @pl.when(has(way) & sends)
                def _():
                    hop(way, b, i).wait_send()
        return 0

    lax.fori_loop(0, chunks, finish, 0)


def fused(planes, state_matrix, gram_factor):
    block_rows, block_cols = state_matrix.shape
    size = block_cols // 4
    chunks = block_rows // size
    factor_rows, half = gram_factor.shape
    rank = 2 * half
    piece = block_rows // (planes * 4)
    per_row = block_rows // block_cols
    f32, bf16 = jnp.float32, jnp.bfloat16
    dma = pltpu.SemaphoreType.DMA
    scratch = [
        pltpu.VMEM((planes, block_rows, size), f32),
        pltpu.VMEM((size, planes * size), bf16),
        pltpu.VMEM((size, planes * size), bf16),
        pltpu.VMEM((per_row, 4, size, size), f32),
        pltpu.VMEM((2, planes * size, 2 * size), bf16),
        pltpu.VMEM((2, planes * size, 2 * size), bf16),
        pltpu.VMEM((2, 2, 2, size, size), f32),
        pltpu.VMEM((chunks, 2, size, size), f32),
        pltpu.VMEM((chunks, size, size), f32),
        pltpu.VMEM((factor_rows, rank), f32),
        pltpu.VMEM((factor_rows, rank), bf16),
        pltpu.VMEM((factor_rows, rank), bf16),
        pltpu.VMEM((planes, 2, 2, piece, rank), f32),
        pltpu.VMEM((planes, 2, piece, rank), f32),
        pltpu.VMEM((planes, piece, rank), f32),
        pltpu.VMEM((planes, piece, rank), f32),
        pltpu.VMEM((4, 8, rank), f32),
        pltpu.VMEM((3, 8, rank), f32),
        pltpu.VMEM((planes, 8, rank), f32),
        dma((chunks,)), dma((per_row, 4)), dma((chunks,)), dma((1,)),
        dma((2, planes, chunks)), dma((planes, chunks)),
        dma((per_row, 4)), dma((per_row, 4)),
        dma((chunks,)), dma((chunks,)), dma((chunks,)), dma((chunks,)),
        dma((6,)), dma((6,)), dma((planes,)), dma((planes,)), dma((planes,)), dma((planes,)),
    ]
    squared, appended, norm = pl.pallas_call(
        functools.partial(kernel, planes),
        out_shape=[
            jax.ShapeDtypeStruct((block_rows, size), f32),
            jax.ShapeDtypeStruct((piece, rank), f32),
            jax.ShapeDtypeStruct((1, rank), f32),
        ],
        in_specs=[pl.BlockSpec(memory_space=pl.ANY)] * 2,
        out_specs=[
            pl.BlockSpec(memory_space=pl.ANY),
            pl.BlockSpec(memory_space=pltpu.VMEM),
            pl.BlockSpec(memory_space=pltpu.VMEM),
        ],
        scratch_shapes=scratch,
        compiler_params=pltpu.CompilerParams(has_side_effects=True, vmem_limit_bytes=VMEM_BYTES),
    )(state_matrix, gram_factor)
    return squared, appended, norm[0]


def product(left, right):
    return jnp.dot(left, right, preferred_element_type=jnp.float32, precision=lax.Precision.HIGH)


def halving_order(count):
    order = [0]
    step = 1
    while step < count:
        order = [2 * j for j in order] + [2 * j + 1 for j in order]
        step *= 2
    return order


def exchange(value, bit, count):
    return lax.ppermute(value, "depth", [(d, d ^ bit) for d in range(count)])


def body(state_matrix, gram_factor):
    row_count = lax.axis_size("row")
    col_count = lax.axis_size("col")
    depth_count = lax.axis_size("depth")
    row_index = lax.axis_index("row")
    col_index = lax.axis_index("col")
    depth_index = lax.axis_index("depth")
    block_rows, block_cols = state_matrix.shape
    slab = block_cols // depth_count
    blocks_per_row = block_rows // block_cols
    order = halving_order(depth_count)

    own_columns = lax.dynamic_slice_in_dim(state_matrix, depth_index * slab, slab, 1)
    edges = [block_rows * part // 16 for part in (0, 7, 13, 16)]
    lefts = [
        lax.all_gather(own_columns[low:high], "col", axis=1, tiled=True) for low, high in zip(edges, edges[1:])
    ]

    stacked = state_matrix.reshape(blocks_per_row, block_cols, block_cols)
    own_rows = lax.dynamic_slice_in_dim(stacked, depth_index * slab, slab, 1).reshape(
        blocks_per_row * slab, block_cols
    )
    own_rows = jnp.concatenate(
        [lax.dynamic_slice_in_dim(own_rows, (depth_index ^ j) * slab, slab, 1) for j in order], axis=1
    )

    def row_gather(value):
        pieces = [value]
        for s in range(1, row_count):
            pieces.append(lax.ppermute(value, "row", [(r, (r + s) % row_count) for r in range(row_count)]))
        ordered = []
        for r in range(row_count):
            piece = pieces[0]
            for s in range(1, row_count):
                piece = jnp.where(lax.rem(row_index + (row_count - r), row_count) == s, pieces[s], piece)
            ordered.append(piece)
        return ordered

    factor_block = jnp.concatenate(row_gather(gram_factor), axis=1)
    column_block = jnp.concatenate(row_gather(own_rows), axis=0)

    terms = product(own_columns, factor_block)
    piece_rows = block_rows // (col_count * depth_count)
    terms = terms.reshape(col_count, depth_count, piece_rows, terms.shape[1])
    held = jnp.concatenate(
        [lax.dynamic_slice_in_dim(terms, depth_index ^ j, 1, 1) for j in order], axis=1
    )
    bit, width = 1, depth_count
    while width > 1:
        width //= 2
        held = held[:, :width] + exchange(held[:, width:], bit, depth_count)
        bit *= 2
    held = held[:, 0]
    new_rows = lax.dynamic_index_in_dim(held, col_index, 0, keepdims=False)
    for s in range(1, col_count):
        part = lax.dynamic_index_in_dim(held, lax.rem(col_index + s, col_count), 0, keepdims=False)
        new_rows = new_rows + lax.ppermute(part, "col", [(c, (c + s) % col_count) for c in range(col_count)])
    new_sq = jnp.sum(new_rows * new_rows, axis=0)
    old_sq = jnp.sum(factor_block * factor_block, axis=0) * (1.0 / row_count)
    totals_new, totals_old = lax.psum((new_sq, old_sq), ("row", "col", "depth"))
    norm_ratio = jnp.sqrt(totals_new) / jnp.sqrt(totals_old + 1e-06)

    half = block_cols // 2
    outs = []
    for left in lefts:
        if outs:
            left, outs[-1], norm_ratio = lax.optimization_barrier((left, outs[-1], norm_ratio))
        if depth_count == 1:
            outs.append(product(left, column_block))
            continue
        sent = exchange(product(left, column_block[:, half:]), 1, depth_count)
        total = product(left, column_block[:, :half]) + sent
        bit, width = 2, half
        while width > slab:
            width //= 2
            total = total[:, :width] + exchange(total[:, width:], bit, depth_count)
            bit *= 2
        outs.append(total)
    squared = jnp.concatenate(outs, axis=0)
    return (squared, new_rows, norm_ratio)


def solution(mesh):
    in_specs = (P("row", "col"), P(("col", "depth"), "row"))
    out_specs = (P("row", ("col", "depth")), P(("row", "col", "depth"), None), P())

    def run(state_matrix, gram_factor):
        rows, cols = state_matrix.shape
        planes = mesh.shape["col"]
        whole_chunks = rows % cols == 0 and cols % (128 * 4) == 0 and gram_factor.shape[1] % 128 == 0
        paired = mesh.shape["row"] == 2 and mesh.shape["depth"] == 4 and 2 * cols * planes == 4 * rows
        if whole_chunks and paired:
            return fused(planes, state_matrix, gram_factor)
        return body(state_matrix, gram_factor)

    return jax.shard_map(run, mesh=mesh, in_specs=in_specs, out_specs=out_specs, check_vma=False)
```

```python
import functools

import jax
import jax.numpy as jnp
from jax import lax
from jax.experimental import pallas as pl
from jax.experimental.pallas import tpu as pltpu
from jax.sharding import PartitionSpec as P


MESH = pl.DeviceIdType.MESH
VMEM_BYTES = 66_900_000


def split(value):
    high = value.astype(jnp.bfloat16)
    return high, (value - high.astype(jnp.float32)).astype(jnp.bfloat16)


def dot(left, right):
    return jnp.dot(left, right, preferred_element_type=jnp.float32)


def kernel(
    planes, aided, a_hbm, z_hbm, sq_hbm, app_ref, norm_ref, aid_hbm,
    left, left_hi, left_lo, far_rows, right_hi, right_lo, aid_hi, aid_lo, part, got_core, got_x,
    fac, fac_hi, fac_lo, terms, t_core, t_x, t_z, sums, s_got, s_z,
    own_sem, rows_sem, out_sem, fac_own_sem, z_send, z_recv, y_send, y_recv, core_send, core_recv,
    x_send, x_recv, small_send, small_recv, tz_send, tz_recv, sz_send, sz_recv,
    aid_send, aid_recv, aid_y_send, aid_y_recv, give_send, give_recv, credit,
):
    y, c, d = lax.axis_index("row"), lax.axis_index("col"), lax.axis_index("depth")
    x, k = lax.div(d, 2), lax.rem(d, 2)
    core_mate = {"depth": d + 1 - 2 * k}
    x_mate = {"depth": lax.rem(d + 2, 4)}
    y_mate = {"row": 1 - y}
    tall, size = part.shape[3:]
    chunks = left.shape[1] // tall
    lead = 1
    first = chunks // 2
    early = first + first // 2
    ring = got_core.shape[0]
    per_row = a_hbm.shape[0] // a_hbm.shape[1]
    block = a_hbm.shape[1]
    inner = (c > 0) & (c < planes - 1)
    outer = jnp.logical_not(inner)
    own_cols = pl.ds(pl.multiple_of(d * size, size), size)
    low = 1 - lax.div(c, 2)
    minor = lax.rem(y + low, 2)
    aid_to = {"col": 3 - 3 * low}
    aid_from = {"col": 2 - low}
    near_b, mid_b, far_b = 2 - low, 1 + low, 3 * low
    first_b = far_b + (near_b - far_b) * minor
    other_b = near_b + (far_b - near_b) * minor

    def rows(i):
        return pl.ds(pl.multiple_of(i * tall, tall), tall)

    def remote(src, dst, send, recv, target):
        return pltpu.make_async_remote_copy(
            src_ref=src, dst_ref=dst, send_sem=send, recv_sem=recv, device_id=target, device_id_type=MESH
        )

    def hop(way, b, i, own=False):
        src = a_hbm.at[rows(i), own_cols] if own else left.at[b, rows(i)]
        target = {"col": c + 1 - 2 * way}
        return remote(src, left.at[b, rows(i)], z_send.at[way, b, i], z_recv.at[b, i], target)

    def shared(i):
        return (i < lead) | (i >= lead + aided)

    def goes(way, i):
        if way == 0:
            return (c < planes - 2) | ((c == planes - 2) & shared(i))
        return (c > 1) | ((c == 1) & shared(i))

    def send_own(i, ways=(0, 1)):
        for way in ways:
            @pl.when(goes(way, i))
            def _():
                hop(way, c, i, own=True).start()

    def to_center(i):
        pl.when(low == 1)(lambda: send_own(i, (0,)))
        pl.when(low == 0)(lambda: send_own(i, (1,)))

    def to_end(i):
        pl.when(low == 1)(lambda: send_own(i, (1,)))
        pl.when(low == 0)(lambda: send_own(i, (0,)))

    def arrivals(i):
        for b in range(planes):
            @pl.when(b != c)
            def _():
                hop(0, b, i).wait_recv()

    def pass_on(way, b, i):
        hop(way, b, i).wait_recv()
        @pl.when(goes(way, i))
        def _():
            hop(way, b, i).start()

    def came_out(i):
        pl.when(low == 1)(lambda: pass_on(0, 0, i))
        pl.when(low == 0)(lambda: pass_on(1, planes - 1, i))

    def came_in(i):
        pl.when(low == 1)(lambda: pass_on(1, 2, i))
        pl.when(low == 0)(lambda: pass_on(0, 1, i))

    def came_far(i):
        pl.when(low == 1)(lambda: pass_on(1, planes - 1, i))
        pl.when(low == 0)(lambda: pass_on(0, 0, i))

    def own_copy(i):
        return pltpu.make_async_copy(a_hbm.at[rows(i), own_cols], left.at[c, rows(i)], own_sem.at[i])

    def right_rows(q, j):
        return a_hbm.at[pl.ds(pl.multiple_of(q * block + d * size, size), size), pl.ds(j * size, size)]

    def near_place(q, j):
        return got_x.at[pl.ds((q * 4 + j) * size, size)]

    def near_copy(q, j):
        return pltpu.make_async_copy(right_rows(q, j), near_place(q, j), rows_sem.at[q, j])

    def y_copy(q, j):
        return remote(right_rows(q, j), far_rows.at[q, j], y_send.at[q, j], y_recv.at[q, j], y_mate)

    def aid_copy(b, j, from_far=False):
        q = low if b is first_b else 1 - low
        src = far_rows.at[q, j] if from_far else right_rows(q, j)
        return remote(src, aid_hbm.at[b, j], aid_send.at[b, j], aid_recv.at[b, j], aid_from)

    def aid_y_copy(b, j):
        return remote(aid_hbm.at[b, j], aid_hbm.at[b, j], aid_y_send.at[j], aid_y_recv.at[j], y_mate)

    for i in range(chunks):
        own_copy(i).start()
    for q in range(per_row):
        for j in range(4):
            near_copy(q, j).start()
    barrier = pltpu.get_barrier_semaphore()
    mates = [core_mate, x_mate, y_mate] + [{"col": lax.rem(c + far, planes)} for far in range(1, planes)]
    for mate in mates:
        pl.semaphore_signal(barrier, inc=1, device_id=mate, device_id_type=MESH)
    pl.semaphore_wait(barrier, len(mates))
    half = z_hbm.shape[1]
    lanes = pl.ds(pl.multiple_of(y * half, half), half)
    fac_own = pltpu.make_async_copy(z_hbm, fac.at[:, lanes], fac_own_sem.at[0])
    fac_y = remote(z_hbm, fac.at[:, lanes], small_send.at[0], small_recv.at[0], y_mate)
    fac_y.start()
    fac_own.start()
    @pl.when(inner)
    def _():
        for i in range(first // 2):
            to_center(i)
        for i in range(chunks):
            if not lead <= i < lead + aided:
                to_end(i)
    for j in range(4):
        for q in range(per_row):
            y_copy(q, j).start()
    @pl.when(outer)
    def _():
        for i in range(first):
            send_own(i)
        for j in range(4):
            aid_copy(first_b, j).start()

    def keep_right(high_ref, low_ref, value, j, at):
        high, rest = split(value)
        at = pl.ds(pl.multiple_of(at * size, size), size)
        high_ref[j // 2, at, j % 2 * size : (j % 2 + 1) * size] = high
        low_ref[j // 2, at, j % 2 * size : (j % 2 + 1) * size] = rest

    for i in range(chunks):
        own_copy(i).wait()
    fac_own.wait()
    fac_y.wait_recv()
    fac_hi[...], fac_lo[...] = split(fac[...])
    piece = terms.shape[3]

    def term(i, _):
        high, rest = split(left[c, pl.ds(pl.multiple_of(i * size, size), size)])
        value = dot(high, fac_hi[...]) + dot(high, fac_lo[...]) + dot(rest, fac_hi[...])
        for half_k in (0, 1):
            terms[lax.div(i, 2), lax.rem(i, 2), half_k] = value[half_k * piece : (half_k + 1) * piece]
        return 0

    lax.fori_loop(0, left.shape[1] // size, term, 0)
    for q in range(per_row):
        for j in range(4):
            near_copy(q, j).wait()
            keep_right(right_hi, right_lo, near_place(q, j)[...], j, y * per_row + q)
    t_core_copy = remote(terms.at[:, :, 1 - k], t_core, small_send.at[1], small_recv.at[1], core_mate)
    t_core_copy.start()
    t_core_copy.wait_recv()
    for b in range(planes):
        t_core[b, 0] += terms[b, 0, k]
        t_core[b, 1] += terms[b, 1, k]
    @pl.when(inner)
    def _():
        for i in (0, 1):
            came_out(i)
            came_in(i)
            to_center(i + first // 2)
    t_x_copy = remote(t_core.at[:, 1 - x], t_x, small_send.at[2], small_recv.at[2], x_mate)
    t_x_copy.start()
    t_x_copy.wait_recv()
    for b in range(planes):
        t_x[b] += t_core[b, x]
    @pl.when(inner)
    def _():
        came_far(0)

    def line_copy(way, b, at, src=None):
        target = {"col": c + 1 - 2 * way}
        src = t_z.at[at] if src is None else src
        return remote(src, t_z.at[at], tz_send.at[b], tz_recv.at[at], target)

    def line_send(way, b, own=False):
        src = t_x.at[b] if own else t_z.at[b]
        if way == 0:
            return line_copy(0, b, b, src)
        mine = b == planes - 2 if own else b < 2
        return line_copy(1, b, planes if mine else b, src)

    def line_got(at):
        line_copy(0, 0, at).wait_recv()

    def terms_off():
        @pl.when(low == 1)
        def _():
            for b in range(1, planes):
                line_send(0, b, own=True).start()
        @pl.when(low == 0)
        def _():
            for b in range(planes - 1):
                line_send(1, b, own=True).start()

    def terms_on():
        @pl.when(low == 1)
        def _():
            for b in (1, 2, 3):
                line_got(b)
            for b in (2, 3):
                t_z[b] += t_x[b]
                line_send(0, b).start()
        @pl.when(low == 0)
        def _():
            for at in (0, 1, planes):
                line_got(at)
            for b in (0, 1):
                t_z[b] += t_x[b]
            line_copy(1, 0, 0).start()
            line_send(1, 1).start()

    def terms_in():
        @pl.when(low == 1)
        def _():
            line_got(0)
            line_got(planes)
            t_z[0] += t_x[0]
            line_send(1, 0).start()
            app_ref[...] = t_x[1] + t_z[1] + t_z[planes]
        @pl.when(low == 0)
        def _():
            line_got(2)
            line_got(3)
            t_z[3] += t_x[3]
            line_send(0, 3).start()
            app_ref[...] = t_x[2] + t_z[2] + t_z[planes]

    def terms_last():
        @pl.when(low == 1)
        def _():
            line_got(planes)
            app_ref[...] = t_x[0] + t_z[planes]
        @pl.when(low == 0)
        def _():
            line_got(planes - 1)
            app_ref[...] = t_x[planes - 1] + t_z[planes - 1]

    @pl.when(inner)
    def _():
        for i in range(2, first):
            came_out(i)
            came_in(i)
            to_center(i + first // 2)
            came_far(i - 1)

    for j in range(4):
        for q in range(per_row):
            y_copy(q, j).wait_recv()
            keep_right(right_hi, right_lo, far_rows[q, j], j, (1 - y) * per_row + q)
        @pl.when(outer)
        def _():
            if j < 2:
                send_own(first + 2 * j)
                send_own(first + 2 * j + 1)
            for piece_j in ((), (), (0, 1, 2), (3,))[j]:
                @pl.when(minor == 0)
                def _():
                    aid_copy(mid_b, piece_j).start()
                @pl.when(minor == 1)
                def _():
                    aid_copy(mid_b, piece_j, from_far=True).start()
    @pl.when(outer)
    def _():
        terms_off()
        for i in range(early, chunks):
            send_own(i)
    @pl.when(inner)
    def _():
        for j in range(4):
            aid_copy(first_b, j).wait_recv()
            aid_y_copy(first_b, j).start()

    def s_copy(stage, target):
        return remote(sums.at[stage], s_got.at[stage], small_send.at[3 + stage], small_recv.at[3 + stage], target)

    def sz_copy(far):
        b = lax.rem(c + far, planes)
        return remote(sums.at[3], s_z.at[c], sz_send.at[far - 1], sz_recv.at[c], {"col": b})

    def sz_arrival(b):
        return remote(sums.at[3], s_z.at[b], sz_send.at[0], sz_recv.at[b], {"col": b})

    def small(step):
        if step == 0:
            total = app_ref[...]
            new = jnp.sum(total * total, axis=0, keepdims=True)
            old = jnp.sum(fac[...] * fac[...], axis=0, keepdims=True) * 0.5
            sums[0, 0:1] = new
            sums[0, 1:2] = old
            s_copy(0, core_mate).start()
        elif step == 1:
            s_copy(0, core_mate).wait_recv()
            sums[1, 0:2] = sums[0, 0:2] + s_got[0, 0:2]
            s_copy(1, x_mate).start()
        elif step == 2:
            s_copy(1, x_mate).wait_recv()
            sums[2, 0:2] = sums[1, 0:2] + s_got[1, 0:2]
            s_copy(2, y_mate).start()
        elif step == 3:
            s_copy(2, y_mate).wait_recv()
            sums[3, 0:2] = sums[2, 0:2] + s_got[2, 0:2]
            for far in range(1, planes):
                sz_copy(far).start()
        elif step == 4:
            for b in range(planes):
                @pl.when(b != c)
                def _():
                    sz_arrival(b).wait_recv()
            s_z[c, 0:2] = sums[3, 0:2]
            both = s_z[0, 0:2]
            for b in range(1, planes):
                both = both + s_z[b, 0:2]
            norm_ref[...] = jnp.sqrt(both[0:1]) / jnp.sqrt(both[1:2] + 1e-06)

    def core_copy(t):
        return remote(
            part.at[lax.rem(t, 2), :, 1 - k], got_core.at[lax.rem(t, ring)], core_send.at[t], core_recv.at[t], core_mate
        )

    def x_copy(t):
        return remote(got_core.at[lax.rem(t, ring), 1 - x], got_x.at[rows(t)], x_send.at[t], x_recv.at[t], x_mate)

    def out_copy(t, i):
        return pltpu.make_async_copy(got_x.at[rows(t)], sq_hbm.at[rows(i)], out_sem.at[i])

    def give_copy(g):
        return remote(got_x.at[rows(early + g)], got_x.at[rows(chunks + g)], give_send.at[g], give_recv.at[g], aid_to)

    def take_left(at, b, i):
        high, rest = split(left[b, rows(i)])
        left_hi[:, at * size : (at + 1) * size] = high
        left_lo[:, at * size : (at + 1) * size] = rest

    def multiply(t, width, high_ref, low_ref):
        def side(s, _):
            high, rest = left_hi[:, :width], left_lo[:, :width]
            value = dot(high, high_ref[s]) + dot(high, low_ref[s]) + dot(rest, high_ref[s])
            part[lax.rem(t, 2), s, 0] = value[:, :size]
            part[lax.rem(t, 2), s, 1] = value[:, size:]
            return 0

        lax.fori_loop(0, 2, side, 0)

    def after_core(t):
        core_copy(t).wait_recv()
        at = lax.rem(t, ring)
        got_core[at, 1 - x] += part[lax.rem(t, 2), 1 - x, k]
        got_core[at, x] += part[lax.rem(t, 2), x, k]
        x_copy(t).start()

    def after_x(t, last):
        x_copy(t).wait_recv()
        got_x[rows(t)] += got_core[lax.rem(t, ring), x]
        x_copy(t).wait_send()
        @pl.when(t + ring <= last)
        def _():
            pl.semaphore_signal(credit, inc=1, device_id=core_mate, device_id_type=MESH)

    def slot(t, last, fill, deliver):
        @pl.when(t >= 2)
        def _():
            core_copy(t - 2).wait_send()
        fill()
        @pl.when(t >= 1)
        def _():
            after_core(t - 1)
        @pl.when(t >= ring)
        def _():
            pl.semaphore_wait(credit, 1)
        core_copy(t).start()
        @pl.when(t >= 2)
        def _():
            after_x(t - 2, last)
            deliver(t - 2)

    def drain(last, deliver):
        after_core(last)
        after_x(last - 1, last)
        deliver(last - 1)
        small(2)
        small(3)
        after_x(last, last)
        deliver(last)
        core_copy(last - 1).wait_send()
        core_copy(last).wait_send()

    @pl.when(outer)
    def _():
        last = chunks - 1

        def place(t):
            return t - aided + aided * lax.div(t + chunks - lead - aided, chunks)

        def deliver(t):
            @pl.when(t >= aided)
            def _():
                out_copy(t, place(t)).start()

        def step(t, _):
            def alone():
                for b in range(planes):
                    @pl.when(b == c)
                    def _():
                        take_left(b, b, lead + t)
                    @pl.when(b != c)
                    def _():
                        left_hi[:, b * size : (b + 1) * size] = jnp.zeros((tall, size), jnp.bfloat16)
                        left_lo[:, b * size : (b + 1) * size] = jnp.zeros((tall, size), jnp.bfloat16)

            def whole():
                arrivals(place(t))
                for b in range(planes):
                    take_left(b, b, place(t))

            def fill():
                pl.when(t < aided)(alone)
                pl.when(t >= aided)(whole)
                multiply(t, planes * size, right_hi, right_lo)

            @pl.when(t == last)
            def _():
                terms_last()
                small(0)
            slot(t, last, fill, deliver)
            @pl.when(t == last)
            def _():
                small(1)
            return 0

        lax.fori_loop(0, chunks, step, 0)
        drain(last, deliver)
        for g in range(aided):
            give_copy(g).wait_recv()
            got_x[rows(g)] += got_x[rows(chunks + g)]
            out_copy(g, lead + g).start()
        for i in range(chunks):
            out_copy(0, i).wait()
        for j in range(4):
            aid_copy(first_b, j).wait_send()
            aid_copy(mid_b, j).wait_send()

    @pl.when(inner)
    def _():
        last = chunks + aided - 1

        def deliver(t):
            @pl.when(t < early)
            def _():
                out_copy(t, t).start()
            @pl.when(t >= early + aided)
            def _():
                out_copy(t, t - aided).start()

        def take_aid():
            def stage(b, j, at):
                return pltpu.make_async_copy(aid_hbm.at[b, j], far_rows.at[at // 4, at % 4], rows_sem.at[at // 4, at % 4])

            for j in range(4):
                aid_copy(mid_b, j).wait_recv()
                stage(first_b, j, j).start()
                stage(mid_b, j, 4 + j).start()
            for j in range(4):
                stage(first_b, j, j).wait()
                keep_right(aid_hi, aid_lo, far_rows[0, j], j, first_b - low)
                aid_y_copy(other_b, j).wait_recv()
                stage(other_b, j, j).start()
            for j in range(4):
                stage(mid_b, j, 4 + j).wait()
                keep_right(aid_hi, aid_lo, far_rows[1, j], j, mid_b - low)
            for j in range(4):
                stage(other_b, j, j).wait()
                keep_right(aid_hi, aid_lo, far_rows[0, j], j, other_b - low)

        def step(t, _):
            def events(at):
                if at == 1:
                    came_out(first)
                    came_in(first)
                elif at == 2:
                    came_out(first + 1)
                    came_in(first + 1)
                    came_far(first - 1)
                elif at == 3:
                    came_out(first + 2)
                    came_in(first + 2)
                elif at == 4:
                    came_out(first + 3)
                    came_in(first + 3)
                    for i in range(early, chunks):
                        to_center(i)
                elif at < 9:
                    came_far(at + 3)
                elif at < early:
                    came_in(at + 3)
                elif at == early:
                    came_in(chunks - 1)
                    take_aid()
                elif at == early + 2:
                    came_out(early)
                else:
                    came_out(at - 2)
                    came_far(at - 3)

            for at in (*range(1, early + 1), *range(early + 2, chunks + 2)):
                pl.when(t == at)(functools.partial(events, at))
            @pl.when(t == chunks + 2)
            def _():
                came_far(chunks - 1)
                for g in range(aided):
                    give_copy(g).start()

            def fill():
                @pl.when((t >= early) & (t < early + aided))
                def _():
                    for at in range(planes - 1):
                        take_left(at, at + low, t - early + lead)
                    multiply(t, (planes - 1) * size, aid_hi, aid_lo)

                @pl.when((t < early) | (t >= early + aided))
                def _():
                    i = t - aided * lax.div(t, early + aided)
                    for b in range(planes):
                        take_left(b, b, i)
                    multiply(t, planes * size, right_hi, right_lo)

            slot(t, last, fill, deliver)
            @pl.when(t == last - 2)
            def _():
                terms_on()
            @pl.when(t == last - 1)
            def _():
                terms_in()
                small(0)
            @pl.when(t == last)
            def _():
                small(1)
            return 0

        lax.fori_loop(0, chunks + aided, step, 0)
        drain(last, deliver)
        for i in range(chunks):
            out_copy(0, i).wait()
        for g in range(aided):
            give_copy(g).wait_send()
        for j in range(4):
            aid_y_copy(first_b, j).wait_send()

    small(4)

    fac_y.wait_send()
    t_core_copy.wait_send()
    t_x_copy.wait_send()
    for far in range(1, planes):
        sz_copy(far).wait_send()
    for b in range(planes):
        @pl.when(b != c)
        def _():
            line_copy(0, b, b).wait_send()
    for stage, mate in enumerate((core_mate, x_mate, y_mate)):
        s_copy(stage, mate).wait_send()
    for q in range(per_row):
        for j in range(4):
            y_copy(q, j).wait_send()

    def finish(i, _):
        for b in range(planes):
            for way in (0, 1):
                sends = (b <= c) if way == 0 else (b >= c)
                @pl.when(goes(way, i) & sends)
                def _():
                    hop(way, b, i).wait_send()
        return 0

    lax.fori_loop(0, chunks, finish, 0)


def fused(planes, state_matrix, gram_factor):
    block_rows, block_cols = state_matrix.shape
    size = block_cols // 4
    tall = size // 2
    chunks = block_rows // tall
    aided = chunks // 4
    ring = 4
    factor_rows, half = gram_factor.shape
    rank = 2 * half
    piece = block_rows // (planes * 4)
    per_row = block_rows // block_cols
    f32, bf16 = jnp.float32, jnp.bfloat16
    dma = pltpu.SemaphoreType.DMA
    scratch = [
        pltpu.VMEM((planes, block_rows, size), f32),
        pltpu.VMEM((tall, planes * size), bf16),
        pltpu.VMEM((tall, planes * size), bf16),
        pltpu.VMEM((per_row, 4, size, size), f32),
        pltpu.VMEM((2, planes * size, 2 * size), bf16),
        pltpu.VMEM((2, planes * size, 2 * size), bf16),
        pltpu.VMEM((2, (planes - 1) * size, 2 * size), bf16),
        pltpu.VMEM((2, (planes - 1) * size, 2 * size), bf16),
        pltpu.VMEM((2, 2, 2, tall, size), f32),
        pltpu.VMEM((ring, 2, tall, size), f32),
        pltpu.VMEM(((chunks + aided) * tall, size), f32),
        pltpu.VMEM((factor_rows, rank), f32),
        pltpu.VMEM((factor_rows, rank), bf16),
        pltpu.VMEM((factor_rows, rank), bf16),
        pltpu.VMEM((planes, 2, 2, piece, rank), f32),
        pltpu.VMEM((planes, 2, piece, rank), f32),
        pltpu.VMEM((planes, piece, rank), f32),
        pltpu.VMEM((planes + 1, piece, rank), f32),
        pltpu.VMEM((4, 8, rank), f32),
        pltpu.VMEM((3, 8, rank), f32),
        pltpu.VMEM((planes, 8, rank), f32),
        dma((chunks,)), dma((per_row, 4)), dma((chunks,)), dma((1,)),
        dma((2, planes, chunks)), dma((planes, chunks)),
        dma((per_row, 4)), dma((per_row, 4)),
        dma((chunks + aided,)), dma((chunks + aided,)), dma((chunks + aided,)), dma((chunks + aided,)),
        dma((6,)), dma((6,)), dma((planes,)), dma((planes + 1,)), dma((planes,)), dma((planes,)),
        dma((planes, 4)), dma((planes, 4)), dma((4,)), dma((4,)), dma((aided,)), dma((aided,)),
        pltpu.SemaphoreType.REGULAR,
    ]
    squared, appended, norm, _ = pl.pallas_call(
        functools.partial(kernel, planes, aided),
        out_shape=[
            jax.ShapeDtypeStruct((block_rows, size), f32),
            jax.ShapeDtypeStruct((piece, rank), f32),
            jax.ShapeDtypeStruct((1, rank), f32),
            jax.ShapeDtypeStruct((planes, 4, size, size), f32),
        ],
        in_specs=[pl.BlockSpec(memory_space=pl.ANY)] * 2,
        out_specs=[
            pl.BlockSpec(memory_space=pl.ANY),
            pl.BlockSpec(memory_space=pltpu.VMEM),
            pl.BlockSpec(memory_space=pltpu.VMEM),
            pl.BlockSpec(memory_space=pl.ANY),
        ],
        scratch_shapes=scratch,
        compiler_params=pltpu.CompilerParams(collective_id=0, has_side_effects=True, vmem_limit_bytes=VMEM_BYTES),
    )(state_matrix, gram_factor)
    return squared, appended, norm[0]


def product(left, right):
    return jnp.dot(left, right, preferred_element_type=jnp.float32, precision=lax.Precision.HIGH)


def halving_order(count):
    order = [0]
    step = 1
    while step < count:
        order = [2 * j for j in order] + [2 * j + 1 for j in order]
        step *= 2
    return order


def exchange(value, bit, count):
    return lax.ppermute(value, "depth", [(d, d ^ bit) for d in range(count)])


def body(state_matrix, gram_factor):
    row_count = lax.axis_size("row")
    col_count = lax.axis_size("col")
    depth_count = lax.axis_size("depth")
    row_index = lax.axis_index("row")
    col_index = lax.axis_index("col")
    depth_index = lax.axis_index("depth")
    block_rows, block_cols = state_matrix.shape
    slab = block_cols // depth_count
    blocks_per_row = block_rows // block_cols
    order = halving_order(depth_count)

    own_columns = lax.dynamic_slice_in_dim(state_matrix, depth_index * slab, slab, 1)
    edges = [block_rows * part // 16 for part in (0, 7, 13, 16)]
    lefts = [
        lax.all_gather(own_columns[low:high], "col", axis=1, tiled=True) for low, high in zip(edges, edges[1:])
    ]

    stacked = state_matrix.reshape(blocks_per_row, block_cols, block_cols)
    own_rows = lax.dynamic_slice_in_dim(stacked, depth_index * slab, slab, 1).reshape(
        blocks_per_row * slab, block_cols
    )
    own_rows = jnp.concatenate(
        [lax.dynamic_slice_in_dim(own_rows, (depth_index ^ j) * slab, slab, 1) for j in order], axis=1
    )

    def row_gather(value):
        pieces = [value]
        for s in range(1, row_count):
            pieces.append(lax.ppermute(value, "row", [(r, (r + s) % row_count) for r in range(row_count)]))
        ordered = []
        for r in range(row_count):
            piece = pieces[0]
            for s in range(1, row_count):
                piece = jnp.where(lax.rem(row_index + (row_count - r), row_count) == s, pieces[s], piece)
            ordered.append(piece)
        return ordered

    factor_block = jnp.concatenate(row_gather(gram_factor), axis=1)
    column_block = jnp.concatenate(row_gather(own_rows), axis=0)

    terms = product(own_columns, factor_block)
    piece_rows = block_rows // (col_count * depth_count)
    terms = terms.reshape(col_count, depth_count, piece_rows, terms.shape[1])
    held = jnp.concatenate(
        [lax.dynamic_slice_in_dim(terms, depth_index ^ j, 1, 1) for j in order], axis=1
    )
    bit, width = 1, depth_count
    while width > 1:
        width //= 2
        held = held[:, :width] + exchange(held[:, width:], bit, depth_count)
        bit *= 2
    held = held[:, 0]
    new_rows = lax.dynamic_index_in_dim(held, col_index, 0, keepdims=False)
    for s in range(1, col_count):
        part = lax.dynamic_index_in_dim(held, lax.rem(col_index + s, col_count), 0, keepdims=False)
        new_rows = new_rows + lax.ppermute(part, "col", [(c, (c + s) % col_count) for c in range(col_count)])
    new_sq = jnp.sum(new_rows * new_rows, axis=0)
    old_sq = jnp.sum(factor_block * factor_block, axis=0) * (1.0 / row_count)
    totals_new, totals_old = lax.psum((new_sq, old_sq), ("row", "col", "depth"))
    norm_ratio = jnp.sqrt(totals_new) / jnp.sqrt(totals_old + 1e-06)

    half = block_cols // 2
    outs = []
    for left in lefts:
        if outs:
            left, outs[-1], norm_ratio = lax.optimization_barrier((left, outs[-1], norm_ratio))
        if depth_count == 1:
            outs.append(product(left, column_block))
            continue
        sent = exchange(product(left, column_block[:, half:]), 1, depth_count)
        total = product(left, column_block[:, :half]) + sent
        bit, width = 2, half
        while width > slab:
            width //= 2
            total = total[:, :width] + exchange(total[:, width:], bit, depth_count)
            bit *= 2
        outs.append(total)
    squared = jnp.concatenate(outs, axis=0)
    return (squared, new_rows, norm_ratio)


def solution(mesh):
    in_specs = (P("row", "col"), P(("col", "depth"), "row"))
    out_specs = (P("row", ("col", "depth")), P(("row", "col", "depth"), None), P())

    def run(state_matrix, gram_factor):
        rows, cols = state_matrix.shape
        planes = mesh.shape["col"]
        whole_chunks = rows % cols == 0 and cols % (128 * 4) == 0 and gram_factor.shape[1] % 128 == 0
        paired = mesh.shape["row"] == 2 and mesh.shape["depth"] == 4 and planes == 4 and 2 * cols == rows
        if whole_chunks and paired:
            return fused(planes, state_matrix, gram_factor)
        return body(state_matrix, gram_factor)

    return jax.shard_map(run, mesh=mesh, in_specs=in_specs, out_specs=out_specs, check_vma=False)
```

```python
import functools

import jax
import jax.numpy as jnp
from jax import lax
from jax.experimental import pallas as pl
from jax.experimental.pallas import tpu as pltpu
from jax.sharding import PartitionSpec as P


MESH = pl.DeviceIdType.MESH
VMEM_BYTES = 66_900_000


def split(value):
    high = value.astype(jnp.bfloat16)
    return high, (value - high.astype(jnp.float32)).astype(jnp.bfloat16)


def dot(left, right):
    return jnp.dot(left, right, preferred_element_type=jnp.float32)


def kernel(
    planes, aided, a_hbm, z_hbm, sq_hbm, app_ref, norm_ref, aid_hbm,
    left, left_hi, left_lo, far_rows, right_hi, right_lo, aid_hi, aid_lo, part, got_core, got_x,
    fac, fac_hi, fac_lo, terms, t_core, t_x, t_z, sums, s_got, s_z,
    own_sem, rows_sem, out_sem, fac_own_sem, z_send, z_recv, y_send, y_recv, core_send, core_recv,
    x_send, x_recv, small_send, small_recv, tz_send, tz_recv, sz_send, sz_recv,
    aid_send, aid_recv, aid_y_send, aid_y_recv, give_send, give_recv, credit,
):
    y, c, d = lax.axis_index("row"), lax.axis_index("col"), lax.axis_index("depth")
    x, k = lax.div(d, 2), lax.rem(d, 2)
    core_mate = {"depth": d + 1 - 2 * k}
    x_mate = {"depth": lax.rem(d + 2, 4)}
    y_mate = {"row": 1 - y}
    tall, size = part.shape[3:]
    chunks = left.shape[1] // tall
    lead = 1
    first = chunks // 2
    early = first
    ring = got_core.shape[0]
    lag = ring - 2
    per_row = a_hbm.shape[0] // a_hbm.shape[1]
    block = a_hbm.shape[1]
    inner = (c > 0) & (c < planes - 1)
    outer = jnp.logical_not(inner)
    own_cols = pl.ds(pl.multiple_of(d * size, size), size)
    low = 1 - lax.div(c, 2)
    minor = lax.rem(y + low, 2)
    aid_to = {"col": 3 - 3 * low}
    aid_from = {"col": 2 - low}
    near_b, mid_b, far_b = 2 - low, 1 + low, 3 * low
    first_b = far_b + (near_b - far_b) * minor
    other_b = near_b + (far_b - near_b) * minor

    def rows(i):
        return pl.ds(pl.multiple_of(i * tall, tall), tall)

    def remote(src, dst, send, recv, target):
        return pltpu.make_async_remote_copy(
            src_ref=src, dst_ref=dst, send_sem=send, recv_sem=recv, device_id=target, device_id_type=MESH
        )

    def hop(way, b, i, own=False):
        src = a_hbm.at[rows(i), own_cols] if own else left.at[b, rows(i)]
        target = {"col": c + 1 - 2 * way}
        return remote(src, left.at[b, rows(i)], z_send.at[way, b, i], z_recv.at[b, i], target)

    def shared(i):
        return (i < lead) | (i >= lead + aided)

    def goes(way, i):
        if way == 0:
            return (c < planes - 2) | ((c == planes - 2) & shared(i))
        return (c > 1) | ((c == 1) & shared(i))

    def send_own(i, ways=(0, 1)):
        for way in ways:
            @pl.when(goes(way, i))
            def _():
                hop(way, c, i, own=True).start()

    def to_center(i):
        pl.when(low == 1)(lambda: send_own(i, (0,)))
        pl.when(low == 0)(lambda: send_own(i, (1,)))

    def to_end(i):
        pl.when(low == 1)(lambda: send_own(i, (1,)))
        pl.when(low == 0)(lambda: send_own(i, (0,)))

    def arrivals(i):
        for b in range(planes):
            @pl.when(b != c)
            def _():
                hop(0, b, i).wait_recv()

    def pass_on(way, b, i):
        hop(way, b, i).wait_recv()
        @pl.when(goes(way, i))
        def _():
            hop(way, b, i).start()

    def came_out(i):
        pl.when(low == 1)(lambda: pass_on(0, 0, i))
        pl.when(low == 0)(lambda: pass_on(1, planes - 1, i))

    def came_in(i):
        pl.when(low == 1)(lambda: pass_on(1, 2, i))
        pl.when(low == 0)(lambda: pass_on(0, 1, i))

    def came_far(i):
        pl.when(low == 1)(lambda: pass_on(1, planes - 1, i))
        pl.when(low == 0)(lambda: pass_on(0, 0, i))

    def own_copy(i):
        return pltpu.make_async_copy(a_hbm.at[rows(i), own_cols], left.at[c, rows(i)], own_sem.at[i])

    def right_rows(q, j):
        return a_hbm.at[pl.ds(pl.multiple_of(q * block + d * size, size), size), pl.ds(j * size, size)]

    def near_place(q, j):
        return got_x.at[pl.ds((q * 4 + j) * size, size)]

    def near_copy(q, j):
        return pltpu.make_async_copy(right_rows(q, j), near_place(q, j), rows_sem.at[q, j])

    def y_copy(q, j):
        return remote(right_rows(q, j), far_rows.at[q, j], y_send.at[q, j], y_recv.at[q, j], y_mate)

    def aid_copy(b, j, from_far=False):
        q = low if b is first_b else 1 - low
        src = far_rows.at[q, j] if from_far else right_rows(q, j)
        return remote(src, aid_hbm.at[b, j], aid_send.at[b, j], aid_recv.at[b, j], aid_from)

    def aid_y_copy(b, j):
        return remote(aid_hbm.at[b, j], aid_hbm.at[b, j], aid_y_send.at[j], aid_y_recv.at[j], y_mate)

    for i in range(chunks):
        own_copy(i).start()
    for q in range(per_row):
        for j in range(4):
            near_copy(q, j).start()
    barrier = pltpu.get_barrier_semaphore()
    mates = [core_mate, x_mate, y_mate] + [{"col": lax.rem(c + far, planes)} for far in range(1, planes)]
    for mate in mates:
        pl.semaphore_signal(barrier, inc=1, device_id=mate, device_id_type=MESH)
    pl.semaphore_wait(barrier, len(mates))
    half = z_hbm.shape[1]
    lanes = pl.ds(pl.multiple_of(y * half, half), half)
    fac_own = pltpu.make_async_copy(z_hbm, fac.at[:, lanes], fac_own_sem.at[0])
    fac_y = remote(z_hbm, fac.at[:, lanes], small_send.at[0], small_recv.at[0], y_mate)
    fac_y.start()
    fac_own.start()
    @pl.when(inner)
    def _():
        for i in range(first // 2):
            to_center(i)
        for i in range(chunks):
            if not lead <= i < lead + aided:
                to_end(i)
    for j in range(4):
        for q in range(per_row):
            y_copy(q, j).start()
    @pl.when(outer)
    def _():
        for i in range(first):
            send_own(i)
        for j in range(4):
            aid_copy(first_b, j).start()

    def keep_right(high_ref, low_ref, value, j, at):
        high, rest = split(value)
        at = pl.ds(pl.multiple_of(at * size, size), size)
        high_ref[j // 2, at, j % 2 * size : (j % 2 + 1) * size] = high
        low_ref[j // 2, at, j % 2 * size : (j % 2 + 1) * size] = rest

    for i in range(chunks):
        own_copy(i).wait()
    fac_own.wait()
    fac_y.wait_recv()
    fac_hi[...], fac_lo[...] = split(fac[...])
    piece = terms.shape[3]

    def term(i, _):
        high, rest = split(left[c, pl.ds(pl.multiple_of(i * size, size), size)])
        value = dot(high, fac_hi[...]) + dot(high, fac_lo[...]) + dot(rest, fac_hi[...])
        for half_k in (0, 1):
            terms[lax.div(i, 2), lax.rem(i, 2), half_k] = value[half_k * piece : (half_k + 1) * piece]
        return 0

    lax.fori_loop(0, left.shape[1] // size, term, 0)
    for q in range(per_row):
        for j in range(4):
            near_copy(q, j).wait()
            keep_right(right_hi, right_lo, near_place(q, j)[...], j, y * per_row + q)
    t_core_copy = remote(terms.at[:, :, 1 - k], t_core, small_send.at[1], small_recv.at[1], core_mate)
    t_core_copy.start()
    t_core_copy.wait_recv()
    for b in range(planes):
        t_core[b, 0] += terms[b, 0, k]
        t_core[b, 1] += terms[b, 1, k]
    @pl.when(inner)
    def _():
        for i in (0, 1):
            came_out(i)
            came_in(i)
            to_center(i + first // 2)
    t_x_copy = remote(t_core.at[:, 1 - x], t_x, small_send.at[2], small_recv.at[2], x_mate)
    t_x_copy.start()
    t_x_copy.wait_recv()
    for b in range(planes):
        t_x[b] += t_core[b, x]
    @pl.when(inner)
    def _():
        came_far(0)

    def line_copy(way, b, at, src=None):
        target = {"col": c + 1 - 2 * way}
        src = t_z.at[at] if src is None else src
        return remote(src, t_z.at[at], tz_send.at[b], tz_recv.at[at], target)

    def line_send(way, b, own=False):
        src = t_x.at[b] if own else t_z.at[b]
        if way == 0:
            return line_copy(0, b, b, src)
        mine = b == planes - 2 if own else b < 2
        return line_copy(1, b, planes if mine else b, src)

    def line_got(at):
        line_copy(0, 0, at).wait_recv()

    def terms_off():
        @pl.when(low == 1)
        def _():
            for b in range(1, planes):
                line_send(0, b, own=True).start()
        @pl.when(low == 0)
        def _():
            for b in range(planes - 1):
                line_send(1, b, own=True).start()

    def terms_on():
        @pl.when(low == 1)
        def _():
            for b in (1, 2, 3):
                line_got(b)
            for b in (2, 3):
                t_z[b] += t_x[b]
                line_send(0, b).start()
        @pl.when(low == 0)
        def _():
            for at in (0, 1, planes):
                line_got(at)
            for b in (0, 1):
                t_z[b] += t_x[b]
            line_copy(1, 0, 0).start()
            line_send(1, 1).start()

    def terms_in():
        @pl.when(low == 1)
        def _():
            line_got(0)
            line_got(planes)
            t_z[0] += t_x[0]
            line_send(1, 0).start()
            app_ref[...] = t_x[1] + t_z[1] + t_z[planes]
        @pl.when(low == 0)
        def _():
            line_got(2)
            line_got(3)
            t_z[3] += t_x[3]
            line_send(0, 3).start()
            app_ref[...] = t_x[2] + t_z[2] + t_z[planes]

    def terms_last():
        @pl.when(low == 1)
        def _():
            line_got(planes)
            app_ref[...] = t_x[0] + t_z[planes]
        @pl.when(low == 0)
        def _():
            line_got(planes - 1)
            app_ref[...] = t_x[planes - 1] + t_z[planes - 1]

    @pl.when(inner)
    def _():
        for i in range(2, first):
            came_out(i)
            came_in(i)
            to_center(i + first // 2)
            came_far(i - 1)
        for i in range(first + first // 2, chunks):
            to_center(i)

    for j in range(4):
        for q in range(per_row):
            y_copy(q, j).wait_recv()
            keep_right(right_hi, right_lo, far_rows[q, j], j, (1 - y) * per_row + q)
        @pl.when(outer)
        def _():
            for piece_j in ((), (), (0, 1, 2), (3,))[j]:
                @pl.when(minor == 0)
                def _():
                    aid_copy(mid_b, piece_j).start()
                @pl.when(minor == 1)
                def _():
                    aid_copy(mid_b, piece_j, from_far=True).start()
    @pl.when(outer)
    def _():
        for i in range(first, first + 2):
            send_own(i)
        terms_off()
        for i in range(first + 2, chunks):
            send_own(i)
    @pl.when(inner)
    def _():
        for j in range(4):
            aid_copy(first_b, j).wait_recv()
            aid_y_copy(first_b, j).start()

    def s_copy(stage, target):
        return remote(sums.at[stage], s_got.at[stage], small_send.at[3 + stage], small_recv.at[3 + stage], target)

    def sz_copy(far):
        b = lax.rem(c + far, planes)
        return remote(sums.at[3], s_z.at[c], sz_send.at[far - 1], sz_recv.at[c], {"col": b})

    def sz_arrival(b):
        return remote(sums.at[3], s_z.at[b], sz_send.at[0], sz_recv.at[b], {"col": b})

    def small(step):
        if step == 0:
            total = app_ref[...]
            new = jnp.sum(total * total, axis=0, keepdims=True)
            old = jnp.sum(fac[...] * fac[...], axis=0, keepdims=True) * 0.5
            sums[0, 0:1] = new
            sums[0, 1:2] = old
            s_copy(0, core_mate).start()
        elif step == 1:
            s_copy(0, core_mate).wait_recv()
            sums[1, 0:2] = sums[0, 0:2] + s_got[0, 0:2]
            s_copy(1, x_mate).start()
        elif step == 2:
            s_copy(1, x_mate).wait_recv()
            sums[2, 0:2] = sums[1, 0:2] + s_got[1, 0:2]
            s_copy(2, y_mate).start()
        elif step == 3:
            s_copy(2, y_mate).wait_recv()
            sums[3, 0:2] = sums[2, 0:2] + s_got[2, 0:2]
            for far in range(1, planes):
                sz_copy(far).start()
        elif step == 4:
            for b in range(planes):
                @pl.when(b != c)
                def _():
                    sz_arrival(b).wait_recv()
            s_z[c, 0:2] = sums[3, 0:2]
            both = s_z[0, 0:2]
            for b in range(1, planes):
                both = both + s_z[b, 0:2]
            norm_ref[...] = jnp.sqrt(both[0:1]) / jnp.sqrt(both[1:2] + 1e-06)

    def core_copy(t):
        return remote(
            part.at[lax.rem(t, 2), :, 1 - k], got_core.at[lax.rem(t, ring)], core_send.at[t], core_recv.at[t], core_mate
        )

    def x_copy(t):
        return remote(got_core.at[lax.rem(t, ring), 1 - x], got_x.at[rows(t)], x_send.at[t], x_recv.at[t], x_mate)

    def out_copy(t, i):
        return pltpu.make_async_copy(got_x.at[rows(t)], sq_hbm.at[rows(i)], out_sem.at[i])

    def give_copy(g):
        return remote(got_x.at[rows(early + g)], got_x.at[rows(chunks + g)], give_send.at[g], give_recv.at[g], aid_to)

    def take_left(at, b, i):
        high, rest = split(left[b, rows(i)])
        left_hi[:, at * size : (at + 1) * size] = high
        left_lo[:, at * size : (at + 1) * size] = rest

    def multiply(t, width, high_ref, low_ref):
        def side(s, _):
            high, rest = left_hi[:, :width], left_lo[:, :width]
            value = dot(high, high_ref[s]) + dot(high, low_ref[s]) + dot(rest, high_ref[s])
            part[lax.rem(t, 2), s, 0] = value[:, :size]
            part[lax.rem(t, 2), s, 1] = value[:, size:]
            return 0

        lax.fori_loop(0, 2, side, 0)

    def after_core(t):
        core_copy(t).wait_recv()
        at = lax.rem(t, ring)
        got_core[at, 1 - x] += part[lax.rem(t, 2), 1 - x, k]
        got_core[at, x] += part[lax.rem(t, 2), x, k]
        x_copy(t).start()

    def after_x(t, last):
        x_copy(t).wait_recv()
        got_x[rows(t)] += got_core[lax.rem(t, ring), x]
        x_copy(t).wait_send()
        @pl.when(t + ring <= last)
        def _():
            pl.semaphore_signal(credit, inc=1, device_id=core_mate, device_id_type=MESH)

    def slot(t, last, fill, deliver):
        @pl.when(t >= 2)
        def _():
            core_copy(t - 2).wait_send()
        fill()
        @pl.when(t >= 1)
        def _():
            after_core(t - 1)
        @pl.when(t >= ring)
        def _():
            pl.semaphore_wait(credit, 1)
        core_copy(t).start()
        @pl.when(t >= lag)
        def _():
            after_x(t - lag, last)
            deliver(t - lag)

    def drain(last, deliver):
        after_core(last)
        for back in range(lag - 1, 0, -1):
            after_x(last - back, last)
            deliver(last - back)
        small(2)
        small(3)
        after_x(last, last)
        deliver(last)
        core_copy(last - 1).wait_send()
        core_copy(last).wait_send()

    @pl.when(outer)
    def _():
        last = chunks - 1

        def place(t):
            return t - aided + aided * lax.div(t + chunks - lead - aided, chunks)

        def deliver(t):
            @pl.when(t >= aided)
            def _():
                out_copy(t, place(t)).start()

        def step(t, _):
            def alone():
                for b in range(planes):
                    @pl.when(b == c)
                    def _():
                        take_left(b, b, lead + t)
                    @pl.when(b != c)
                    def _():
                        left_hi[:, b * size : (b + 1) * size] = jnp.zeros((tall, size), jnp.bfloat16)
                        left_lo[:, b * size : (b + 1) * size] = jnp.zeros((tall, size), jnp.bfloat16)

            def whole():
                arrivals(place(t))
                for b in range(planes):
                    take_left(b, b, place(t))

            def fill():
                pl.when(t < aided)(alone)
                pl.when(t >= aided)(whole)
                multiply(t, planes * size, right_hi, right_lo)

            @pl.when(t == last)
            def _():
                terms_last()
                small(0)
            slot(t, last, fill, deliver)
            @pl.when(t == last)
            def _():
                small(1)
            return 0

        lax.fori_loop(0, chunks, step, 0)
        drain(last, deliver)
        for g in range(aided):
            give_copy(g).wait_recv()
            got_x[rows(g)] += got_x[rows(chunks + g)]
            out_copy(g, lead + g).start()
        for i in range(chunks):
            out_copy(0, i).wait()
        for j in range(4):
            aid_copy(first_b, j).wait_send()
            aid_copy(mid_b, j).wait_send()

    @pl.when(inner)
    def _():
        last = chunks + aided - 1
        keep = 1

        def deliver(t):
            @pl.when(t < early)
            def _():
                out_copy(t, t).start()
            @pl.when((t >= early) & (t < early + keep))
            def _():
                give_copy(t - early).start()
            @pl.when(t >= early + aided)
            def _():
                out_copy(t, t - aided).start()

        def take_aid():
            def stage(b, j, at):
                return pltpu.make_async_copy(aid_hbm.at[b, j], far_rows.at[at // 4, at % 4], rows_sem.at[at // 4, at % 4])

            for j in range(4):
                aid_copy(mid_b, j).wait_recv()
                stage(first_b, j, j).start()
                stage(mid_b, j, 4 + j).start()
            for j in range(4):
                stage(first_b, j, j).wait()
                keep_right(aid_hi, aid_lo, far_rows[0, j], j, first_b - low)
                aid_y_copy(other_b, j).wait_recv()
                stage(other_b, j, j).start()
            for j in range(4):
                stage(mid_b, j, 4 + j).wait()
                keep_right(aid_hi, aid_lo, far_rows[1, j], j, mid_b - low)
            for j in range(4):
                stage(other_b, j, j).wait()
                keep_right(aid_hi, aid_lo, far_rows[0, j], j, other_b - low)

        def step(t, _):
            def events(at):
                if at < first:
                    came_in(first + at - 1)
                    if at == 2:
                        came_far(first - 1)
                elif at == first:
                    came_in(chunks - 1)
                    take_aid()
                    came_out(first)
                elif at == first + 1:
                    came_out(first + 1)
                elif at == first + 2:
                    came_far(first)
                elif at == first + aided - 1:
                    came_far(first + 1)
                elif at == first + aided + 1:
                    came_out(first + 2)
                    came_out(first + 3)
                    came_far(first + 2)
                elif at < last - 1:
                    came_out(at - aided + 2)
                    came_far(at - aided + 1)
                else:
                    came_far(chunks - 1)
                    for g in range(keep, aided):
                        give_copy(g).start()

            for at in (*range(1, first + 3), *range(first + aided - 1, chunks + aided - 1)):
                if at != first + aided:
                    pl.when(t == at)(functools.partial(events, at))

            def fill():
                @pl.when((t >= early) & (t < early + aided))
                def _():
                    for at in range(planes - 1):
                        take_left(at, at + low, t - early + lead)
                    multiply(t, (planes - 1) * size, aid_hi, aid_lo)

                @pl.when((t < early) | (t >= early + aided))
                def _():
                    i = t - aided * lax.div(t, early + aided)
                    for b in range(planes):
                        take_left(b, b, i)
                    multiply(t, planes * size, right_hi, right_lo)

            slot(t, last, fill, deliver)
            @pl.when(t == first + aided)
            def _():
                terms_on()
            @pl.when(t == first + aided + 2)
            def _():
                terms_in()
                small(0)
            @pl.when(t == first + aided + 3)
            def _():
                small(1)
            return 0

        lax.fori_loop(0, chunks + aided, step, 0)
        drain(last, deliver)
        for i in range(chunks):
            out_copy(0, i).wait()
        for g in range(aided):
            give_copy(g).wait_send()
        for j in range(4):
            aid_y_copy(first_b, j).wait_send()

    small(4)

    fac_y.wait_send()
    t_core_copy.wait_send()
    t_x_copy.wait_send()
    for far in range(1, planes):
        sz_copy(far).wait_send()
    for b in range(planes):
        @pl.when(b != c)
        def _():
            line_copy(0, b, b).wait_send()
    for stage, mate in enumerate((core_mate, x_mate, y_mate)):
        s_copy(stage, mate).wait_send()
    for q in range(per_row):
        for j in range(4):
            y_copy(q, j).wait_send()

    def finish(i, _):
        for b in range(planes):
            for way in (0, 1):
                sends = (b <= c) if way == 0 else (b >= c)
                @pl.when(goes(way, i) & sends)
                def _():
                    hop(way, b, i).wait_send()
        return 0

    lax.fori_loop(0, chunks, finish, 0)


def fused(planes, state_matrix, gram_factor):
    block_rows, block_cols = state_matrix.shape
    size = block_cols // 4
    tall = size // 2
    chunks = block_rows // tall
    aided = chunks // 4
    ring = 6
    factor_rows, half = gram_factor.shape
    rank = 2 * half
    piece = block_rows // (planes * 4)
    per_row = block_rows // block_cols
    f32, bf16 = jnp.float32, jnp.bfloat16
    dma = pltpu.SemaphoreType.DMA
    scratch = [
        pltpu.VMEM((planes, block_rows, size), f32),
        pltpu.VMEM((tall, planes * size), bf16),
        pltpu.VMEM((tall, planes * size), bf16),
        pltpu.VMEM((per_row, 4, size, size), f32),
        pltpu.VMEM((2, planes * size, 2 * size), bf16),
        pltpu.VMEM((2, planes * size, 2 * size), bf16),
        pltpu.VMEM((2, (planes - 1) * size, 2 * size), bf16),
        pltpu.VMEM((2, (planes - 1) * size, 2 * size), bf16),
        pltpu.VMEM((2, 2, 2, tall, size), f32),
        pltpu.VMEM((ring, 2, tall, size), f32),
        pltpu.VMEM(((chunks + aided) * tall, size), f32),
        pltpu.VMEM((factor_rows, rank), f32),
        pltpu.VMEM((factor_rows, rank), bf16),
        pltpu.VMEM((factor_rows, rank), bf16),
        pltpu.VMEM((planes, 2, 2, piece, rank), f32),
        pltpu.VMEM((planes, 2, piece, rank), f32),
        pltpu.VMEM((planes, piece, rank), f32),
        pltpu.VMEM((planes + 1, piece, rank), f32),
        pltpu.VMEM((4, 8, rank), f32),
        pltpu.VMEM((3, 8, rank), f32),
        pltpu.VMEM((planes, 8, rank), f32),
        dma((chunks,)), dma((per_row, 4)), dma((chunks,)), dma((1,)),
        dma((2, planes, chunks)), dma((planes, chunks)),
        dma((per_row, 4)), dma((per_row, 4)),
        dma((chunks + aided,)), dma((chunks + aided,)), dma((chunks + aided,)), dma((chunks + aided,)),
        dma((6,)), dma((6,)), dma((planes,)), dma((planes + 1,)), dma((planes,)), dma((planes,)),
        dma((planes, 4)), dma((planes, 4)), dma((4,)), dma((4,)), dma((aided,)), dma((aided,)),
        pltpu.SemaphoreType.REGULAR,
    ]
    squared, appended, norm, _ = pl.pallas_call(
        functools.partial(kernel, planes, aided),
        out_shape=[
            jax.ShapeDtypeStruct((block_rows, size), f32),
            jax.ShapeDtypeStruct((piece, rank), f32),
            jax.ShapeDtypeStruct((1, rank), f32),
            jax.ShapeDtypeStruct((planes, 4, size, size), f32),
        ],
        in_specs=[pl.BlockSpec(memory_space=pl.ANY)] * 2,
        out_specs=[
            pl.BlockSpec(memory_space=pl.ANY),
            pl.BlockSpec(memory_space=pltpu.VMEM),
            pl.BlockSpec(memory_space=pltpu.VMEM),
            pl.BlockSpec(memory_space=pl.ANY),
        ],
        scratch_shapes=scratch,
        compiler_params=pltpu.CompilerParams(collective_id=0, has_side_effects=True, vmem_limit_bytes=VMEM_BYTES),
    )(state_matrix, gram_factor)
    return squared, appended, norm[0]


def product(left, right):
    return jnp.dot(left, right, preferred_element_type=jnp.float32, precision=lax.Precision.HIGH)


def halving_order(count):
    order = [0]
    step = 1
    while step < count:
        order = [2 * j for j in order] + [2 * j + 1 for j in order]
        step *= 2
    return order


def exchange(value, bit, count):
    return lax.ppermute(value, "depth", [(d, d ^ bit) for d in range(count)])


def body(state_matrix, gram_factor):
    row_count = lax.axis_size("row")
    col_count = lax.axis_size("col")
    depth_count = lax.axis_size("depth")
    row_index = lax.axis_index("row")
    col_index = lax.axis_index("col")
    depth_index = lax.axis_index("depth")
    block_rows, block_cols = state_matrix.shape
    slab = block_cols // depth_count
    blocks_per_row = block_rows // block_cols
    order = halving_order(depth_count)

    own_columns = lax.dynamic_slice_in_dim(state_matrix, depth_index * slab, slab, 1)
    edges = [block_rows * part // 16 for part in (0, 7, 13, 16)]
    lefts = [
        lax.all_gather(own_columns[low:high], "col", axis=1, tiled=True) for low, high in zip(edges, edges[1:])
    ]

    stacked = state_matrix.reshape(blocks_per_row, block_cols, block_cols)
    own_rows = lax.dynamic_slice_in_dim(stacked, depth_index * slab, slab, 1).reshape(
        blocks_per_row * slab, block_cols
    )
    own_rows = jnp.concatenate(
        [lax.dynamic_slice_in_dim(own_rows, (depth_index ^ j) * slab, slab, 1) for j in order], axis=1
    )

    def row_gather(value):
        pieces = [value]
        for s in range(1, row_count):
            pieces.append(lax.ppermute(value, "row", [(r, (r + s) % row_count) for r in range(row_count)]))
        ordered = []
        for r in range(row_count):
            piece = pieces[0]
            for s in range(1, row_count):
                piece = jnp.where(lax.rem(row_index + (row_count - r), row_count) == s, pieces[s], piece)
            ordered.append(piece)
        return ordered

    factor_block = jnp.concatenate(row_gather(gram_factor), axis=1)
    column_block = jnp.concatenate(row_gather(own_rows), axis=0)

    terms = product(own_columns, factor_block)
    piece_rows = block_rows // (col_count * depth_count)
    terms = terms.reshape(col_count, depth_count, piece_rows, terms.shape[1])
    held = jnp.concatenate(
        [lax.dynamic_slice_in_dim(terms, depth_index ^ j, 1, 1) for j in order], axis=1
    )
    bit, width = 1, depth_count
    while width > 1:
        width //= 2
        held = held[:, :width] + exchange(held[:, width:], bit, depth_count)
        bit *= 2
    held = held[:, 0]
    new_rows = lax.dynamic_index_in_dim(held, col_index, 0, keepdims=False)
    for s in range(1, col_count):
        part = lax.dynamic_index_in_dim(held, lax.rem(col_index + s, col_count), 0, keepdims=False)
        new_rows = new_rows + lax.ppermute(part, "col", [(c, (c + s) % col_count) for c in range(col_count)])
    new_sq = jnp.sum(new_rows * new_rows, axis=0)
    old_sq = jnp.sum(factor_block * factor_block, axis=0) * (1.0 / row_count)
    totals_new, totals_old = lax.psum((new_sq, old_sq), ("row", "col", "depth"))
    norm_ratio = jnp.sqrt(totals_new) / jnp.sqrt(totals_old + 1e-06)

    half = block_cols // 2
    outs = []
    for left in lefts:
        if outs:
            left, outs[-1], norm_ratio = lax.optimization_barrier((left, outs[-1], norm_ratio))
        if depth_count == 1:
            outs.append(product(left, column_block))
            continue
        sent = exchange(product(left, column_block[:, half:]), 1, depth_count)
        total = product(left, column_block[:, :half]) + sent
        bit, width = 2, half
        while width > slab:
            width //= 2
            total = total[:, :width] + exchange(total[:, width:], bit, depth_count)
            bit *= 2
        outs.append(total)
    squared = jnp.concatenate(outs, axis=0)
    return (squared, new_rows, norm_ratio)


def solution(mesh):
    in_specs = (P("row", "col"), P(("col", "depth"), "row"))
    out_specs = (P("row", ("col", "depth")), P(("row", "col", "depth"), None), P())

    def run(state_matrix, gram_factor):
        rows, cols = state_matrix.shape
        planes = mesh.shape["col"]
        whole_chunks = rows % cols == 0 and cols % (128 * 4) == 0 and gram_factor.shape[1] % 128 == 0
        paired = mesh.shape["row"] == 2 and mesh.shape["depth"] == 4 and planes == 4 and 2 * cols == rows
        if whole_chunks and paired:
            return fused(planes, state_matrix, gram_factor)
        return body(state_matrix, gram_factor)

    return jax.shard_map(run, mesh=mesh, in_specs=in_specs, out_specs=out_specs, check_vma=False)
```

```python
import functools

import jax
import jax.numpy as jnp
from jax import lax
from jax.experimental import pallas as pl
from jax.experimental.pallas import tpu as pltpu
from jax.sharding import PartitionSpec as P


MESH = pl.DeviceIdType.MESH
VMEM_BYTES = 66_900_000


def split(value):
    high = value.astype(jnp.bfloat16)
    return high, (value - high.astype(jnp.float32)).astype(jnp.bfloat16)


def dot(left, right):
    return jnp.dot(left, right, preferred_element_type=jnp.float32)


def kernel(
    planes, aided, a_hbm, z_hbm, sq_hbm, app_hbm, norm_ref, aid_hbm,
    left, left_hi, left_lo, far_rows, right_hi, right_lo, aid_hi, aid_lo, part, got_core, got_x,
    fac, fac_hi, fac_lo, terms, t_core, t_x, t_z, sums, s_got, s_z, app_ref,
    own_sem, rows_sem, out_sem, fac_own_sem, app_sem, z_send, z_recv, y_send, y_recv, core_send, core_recv,
    x_send, x_recv, small_send, small_recv, tz_send, tz_recv, sz_send, sz_recv,
    aid_send, aid_recv, aid_y_send, aid_y_recv, give_send, give_recv, credit,
):
    y, c, d = lax.axis_index("row"), lax.axis_index("col"), lax.axis_index("depth")
    x, k = lax.div(d, 2), lax.rem(d, 2)
    core_mate = {"depth": d + 1 - 2 * k}
    x_mate = {"depth": lax.rem(d + 2, 4)}
    y_mate = {"row": 1 - y}
    tall, size = part.shape[3:]
    chunks = left.shape[1] // tall
    lead = 1
    first = chunks // 2
    early = first
    ring = got_core.shape[0]
    lag = ring - 2
    per_row = a_hbm.shape[0] // a_hbm.shape[1]
    block = a_hbm.shape[1]
    inner = (c > 0) & (c < planes - 1)
    outer = jnp.logical_not(inner)
    own_cols = pl.ds(pl.multiple_of(d * size, size), size)
    low = 1 - lax.div(c, 2)
    minor = lax.rem(y + low, 2)
    aid_to = {"col": 3 - 3 * low}
    aid_from = {"col": 2 - low}
    near_b, mid_b, far_b = 2 - low, 1 + low, 3 * low
    first_b = far_b + (near_b - far_b) * minor
    other_b = near_b + (far_b - near_b) * minor

    def rows(i):
        return pl.ds(pl.multiple_of(i * tall, tall), tall)

    def remote(src, dst, send, recv, target):
        return pltpu.make_async_remote_copy(
            src_ref=src, dst_ref=dst, send_sem=send, recv_sem=recv, device_id=target, device_id_type=MESH
        )

    def hop(way, b, i, own=False):
        src = a_hbm.at[rows(i), own_cols] if own else left.at[b, rows(i)]
        target = {"col": c + 1 - 2 * way}
        line = planes if own and way == 1 else b
        return remote(src, left.at[b, rows(i)], z_send.at[line, i], z_recv.at[b, i], target)

    def shared(i):
        return (i < lead) | (i >= lead + aided)

    def goes(way, i):
        if way == 0:
            return (c < planes - 2) | ((c == planes - 2) & shared(i))
        return (c > 1) | ((c == 1) & shared(i))

    def send_own(i, ways=(0, 1)):
        for way in ways:
            @pl.when(goes(way, i))
            def _():
                hop(way, c, i, own=True).start()

    def to_center(i):
        pl.when(low == 1)(lambda: send_own(i, (0,)))
        pl.when(low == 0)(lambda: send_own(i, (1,)))

    def to_end(i):
        pl.when(low == 1)(lambda: send_own(i, (1,)))
        pl.when(low == 0)(lambda: send_own(i, (0,)))

    def arrivals(i):
        for b in range(planes):
            @pl.when(b != c)
            def _():
                hop(0, b, i).wait_recv()

    def pass_on(way, b, i):
        hop(way, b, i).wait_recv()
        @pl.when(goes(way, i))
        def _():
            hop(way, b, i).start()

    def came_out(i):
        pl.when(low == 1)(lambda: pass_on(0, 0, i))
        pl.when(low == 0)(lambda: pass_on(1, planes - 1, i))

    def came_in(i):
        pl.when(low == 1)(lambda: pass_on(1, 2, i))
        pl.when(low == 0)(lambda: pass_on(0, 1, i))

    def came_far(i):
        pl.when(low == 1)(lambda: pass_on(1, planes - 1, i))
        pl.when(low == 0)(lambda: pass_on(0, 0, i))

    own_copy = pltpu.make_async_copy(a_hbm.at[:, own_cols], left.at[c], own_sem.at[0])

    def right_rows(q, j):
        return a_hbm.at[pl.ds(pl.multiple_of(q * block + d * size, size), size), pl.ds(j * size, size)]

    def near_place(q, j):
        return got_x.at[pl.ds((q * 4 + j) * size, size)]

    def near_copy(q, j):
        return pltpu.make_async_copy(right_rows(q, j), near_place(q, j), rows_sem.at[q, j])

    def y_copy(q, j):
        return remote(right_rows(q, j), far_rows.at[q, j], y_send.at[q, j], y_recv.at[q, j], y_mate)

    def aid_copy(b, j, from_far=False):
        q = low if b is first_b else 1 - low
        src = far_rows.at[q, j] if from_far else right_rows(q, j)
        return remote(src, aid_hbm.at[b, j], aid_send.at[b, j], aid_recv.at[b, j], aid_from)

    def aid_y_copy(b, j):
        return remote(aid_hbm.at[b, j], aid_hbm.at[b, j], aid_y_send.at[j], aid_y_recv.at[j], y_mate)

    own_copy.start()
    for q in range(per_row):
        for j in range(4):
            near_copy(q, j).start()
    barrier = pltpu.get_barrier_semaphore()
    mates = [core_mate, x_mate, y_mate] + [{"col": lax.rem(c + far, planes)} for far in range(1, planes)]
    for mate in mates:
        pl.semaphore_signal(barrier, inc=1, device_id=mate, device_id_type=MESH)
    pl.semaphore_wait(barrier, len(mates))
    half = z_hbm.shape[1]
    lanes = pl.ds(pl.multiple_of(y * half, half), half)
    fac_own = pltpu.make_async_copy(z_hbm, fac.at[:, lanes], fac_own_sem.at[0])
    fac_y = remote(z_hbm, fac.at[:, lanes], small_send.at[0], small_recv.at[0], y_mate)
    fac_y.start()
    fac_own.start()
    @pl.when(inner)
    def _():
        for i in range(first // 2):
            to_center(i)
        for i in range(chunks):
            if not lead <= i < lead + aided:
                to_end(i)
    for j in range(4):
        for q in range(per_row):
            y_copy(q, j).start()
    @pl.when(outer)
    def _():
        for i in range(first):
            send_own(i)
        for j in range(4):
            aid_copy(first_b, j).start()

    def keep_right(high_ref, low_ref, value, j, at):
        high, rest = split(value)
        at = pl.ds(pl.multiple_of(at * size, size), size)
        high_ref[j // 2, at, j % 2 * size : (j % 2 + 1) * size] = high
        low_ref[j // 2, at, j % 2 * size : (j % 2 + 1) * size] = rest

    own_copy.wait()
    fac_own.wait()
    fac_y.wait_recv()
    fac_hi[...], fac_lo[...] = split(fac[...])
    piece = terms.shape[3]

    def term(i, _):
        high, rest = split(left[c, pl.ds(pl.multiple_of(i * size, size), size)])
        value = dot(high, fac_hi[...]) + dot(high, fac_lo[...]) + dot(rest, fac_hi[...])
        for half_k in (0, 1):
            terms[lax.div(i, 2), lax.rem(i, 2), half_k] = value[half_k * piece : (half_k + 1) * piece]
        return 0

    lax.fori_loop(0, left.shape[1] // size, term, 0)
    for q in range(per_row):
        for j in range(4):
            near_copy(q, j).wait()
            keep_right(right_hi, right_lo, near_place(q, j)[...], j, y * per_row + q)
    t_core_copy = remote(terms.at[:, :, 1 - k], t_core, small_send.at[1], small_recv.at[1], core_mate)
    t_core_copy.start()
    t_core_copy.wait_recv()
    for b in range(planes):
        t_core[b, 0] += terms[b, 0, k]
        t_core[b, 1] += terms[b, 1, k]
    @pl.when(inner)
    def _():
        for i in (0, 1):
            came_out(i)
            came_in(i)
            to_center(i + first // 2)
    t_x_copy = remote(t_core.at[:, 1 - x], t_x, small_send.at[2], small_recv.at[2], x_mate)
    t_x_copy.start()
    t_x_copy.wait_recv()
    for b in range(planes):
        t_x[b] += t_core[b, x]
    @pl.when(inner)
    def _():
        came_far(0)

    def line_copy(way, b, at, src=None):
        target = {"col": c + 1 - 2 * way}
        src = t_z.at[at] if src is None else src
        return remote(src, t_z.at[at], tz_send.at[b], tz_recv.at[at], target)

    def line_send(way, b, own=False):
        src = t_x.at[b] if own else t_z.at[b]
        if way == 0:
            return line_copy(0, b, b, src)
        mine = b == planes - 2 if own else b < 2
        return line_copy(1, b, planes if mine else b, src)

    def line_got(at):
        line_copy(0, 0, at).wait_recv()

    def terms_off():
        @pl.when(low == 1)
        def _():
            for b in range(1, planes):
                line_send(0, b, own=True).start()
        @pl.when(low == 0)
        def _():
            for b in range(planes - 1):
                line_send(1, b, own=True).start()

    def terms_on():
        @pl.when(low == 1)
        def _():
            for b in (1, 2, 3):
                line_got(b)
            for b in (2, 3):
                t_z[b] += t_x[b]
                line_send(0, b).start()
        @pl.when(low == 0)
        def _():
            for at in (0, 1, planes):
                line_got(at)
            for b in (0, 1):
                t_z[b] += t_x[b]
            line_copy(1, 0, 0).start()
            line_send(1, 1).start()

    def terms_in():
        @pl.when(low == 1)
        def _():
            line_got(0)
            line_got(planes)
            t_z[0] += t_x[0]
            line_send(1, 0).start()
            app_ref[...] = t_x[1] + t_z[1] + t_z[planes]
        @pl.when(low == 0)
        def _():
            line_got(2)
            line_got(3)
            t_z[3] += t_x[3]
            line_send(0, 3).start()
            app_ref[...] = t_x[2] + t_z[2] + t_z[planes]

    def terms_last():
        @pl.when(low == 1)
        def _():
            line_got(planes)
            app_ref[...] = t_x[0] + t_z[planes]
        @pl.when(low == 0)
        def _():
            line_got(planes - 1)
            app_ref[...] = t_x[planes - 1] + t_z[planes - 1]

    @pl.when(inner)
    def _():
        for i in range(2, first):
            came_out(i)
            came_in(i)
            to_center(i + first // 2)
            came_far(i - 1)
        for i in range(first + first // 2, chunks):
            to_center(i)

    for j in range(4):
        for q in range(per_row):
            y_copy(q, j).wait_recv()
            keep_right(right_hi, right_lo, far_rows[q, j], j, (1 - y) * per_row + q)
        @pl.when(outer)
        def _():
            for piece_j in ((), (), (0, 1, 2), (3,))[j]:
                @pl.when(minor == 0)
                def _():
                    aid_copy(mid_b, piece_j).start()
                @pl.when(minor == 1)
                def _():
                    aid_copy(mid_b, piece_j, from_far=True).start()
    @pl.when(outer)
    def _():
        for i in range(first, first + 2):
            send_own(i)
        terms_off()
        for i in range(first + 2, chunks):
            send_own(i)
    @pl.when(inner)
    def _():
        for j in range(4):
            aid_copy(first_b, j).wait_recv()
            aid_y_copy(first_b, j).start()

    def s_copy(stage, target):
        return remote(sums.at[stage], s_got.at[stage], small_send.at[3 + stage], small_recv.at[3 + stage], target)

    def sz_copy(far):
        b = lax.rem(c + far, planes)
        return remote(sums.at[3], s_z.at[c], sz_send.at[far - 1], sz_recv.at[c], {"col": b})

    def sz_arrival(b):
        return remote(sums.at[3], s_z.at[b], sz_send.at[0], sz_recv.at[b], {"col": b})

    def small(step):
        if step == 0:
            total = app_ref[...]
            pltpu.make_async_copy(app_ref, app_hbm, app_sem.at[0]).start()
            new = jnp.sum(total * total, axis=0, keepdims=True)
            old = jnp.sum(fac[...] * fac[...], axis=0, keepdims=True) * 0.5
            sums[0, 0:1] = new
            sums[0, 1:2] = old
            s_copy(0, core_mate).start()
        elif step == 1:
            s_copy(0, core_mate).wait_recv()
            sums[1, 0:2] = sums[0, 0:2] + s_got[0, 0:2]
            s_copy(1, x_mate).start()
        elif step == 2:
            s_copy(1, x_mate).wait_recv()
            sums[2, 0:2] = sums[1, 0:2] + s_got[1, 0:2]
            s_copy(2, y_mate).start()
        elif step == 3:
            s_copy(2, y_mate).wait_recv()
            sums[3, 0:2] = sums[2, 0:2] + s_got[2, 0:2]
            for far in range(1, planes):
                sz_copy(far).start()
        elif step == 4:
            for b in range(planes):
                @pl.when(b != c)
                def _():
                    sz_arrival(b).wait_recv()
            s_z[c, 0:2] = sums[3, 0:2]
            both = s_z[0, 0:2]
            for b in range(1, planes):
                both = both + s_z[b, 0:2]
            norm_ref[...] = jnp.sqrt(both[0:1]) / jnp.sqrt(both[1:2] + 1e-06)

    def core_copy(t):
        return remote(
            part.at[lax.rem(t, 2), :, 1 - k], got_core.at[lax.rem(t, ring)], core_send.at[t], core_recv.at[t], core_mate
        )

    def x_copy(t):
        return remote(got_core.at[lax.rem(t, ring), 1 - x], got_x.at[rows(t)], x_send.at[t], x_recv.at[t], x_mate)

    def out_copy(t, i):
        return pltpu.make_async_copy(got_x.at[rows(t)], sq_hbm.at[rows(i)], out_sem.at[i])

    def give_copy(g):
        return remote(got_x.at[rows(early + g)], got_x.at[rows(chunks + g)], give_send.at[g], give_recv.at[g], aid_to)

    def take_left(at, b, i):
        high, rest = split(left[b, rows(i)])
        left_hi[:, at * size : (at + 1) * size] = high
        left_lo[:, at * size : (at + 1) * size] = rest

    def multiply(t, width, high_ref, low_ref):
        def side(s, _):
            high, rest = left_hi[:, :width], left_lo[:, :width]
            value = dot(high, high_ref[s]) + dot(high, low_ref[s]) + dot(rest, high_ref[s])
            part[lax.rem(t, 2), s, 0] = value[:, :size]
            part[lax.rem(t, 2), s, 1] = value[:, size:]
            return 0

        lax.fori_loop(0, 2, side, 0)

    def after_core(t):
        core_copy(t).wait_recv()
        at = lax.rem(t, ring)
        got_core[at, 1 - x] += part[lax.rem(t, 2), 1 - x, k]
        got_core[at, x] += part[lax.rem(t, 2), x, k]
        x_copy(t).start()

    def after_x(t, last):
        x_copy(t).wait_recv()
        got_x[rows(t)] += got_core[lax.rem(t, ring), x]
        x_copy(t).wait_send()
        @pl.when(t + ring <= last)
        def _():
            pl.semaphore_signal(credit, inc=1, device_id=core_mate, device_id_type=MESH)

    def slot(t, last, fill, deliver):
        @pl.when(t >= 2)
        def _():
            core_copy(t - 2).wait_send()
        fill()
        @pl.when(t >= 1)
        def _():
            after_core(t - 1)
        @pl.when(t >= ring)
        def _():
            pl.semaphore_wait(credit, 1)
        core_copy(t).start()
        @pl.when(t >= lag)
        def _():
            after_x(t - lag, last)
            deliver(t - lag)

    def drain(last, deliver):
        after_core(last)
        for back in range(lag - 1, 0, -1):
            after_x(last - back, last)
            deliver(last - back)
        small(2)
        small(3)
        after_x(last, last)
        deliver(last)
        core_copy(last - 1).wait_send()
        core_copy(last).wait_send()

    @pl.when(outer)
    def _():
        last = chunks - 1

        def place(t):
            return t - aided + aided * lax.div(t + chunks - lead - aided, chunks)

        def deliver(t):
            @pl.when(t >= aided)
            def _():
                out_copy(t, place(t)).start()

        def step(t, _):
            def alone():
                for b in range(planes):
                    @pl.when(b == c)
                    def _():
                        take_left(b, b, lead + t)
                    @pl.when(b != c)
                    def _():
                        left_hi[:, b * size : (b + 1) * size] = jnp.zeros((tall, size), jnp.bfloat16)
                        left_lo[:, b * size : (b + 1) * size] = jnp.zeros((tall, size), jnp.bfloat16)

            def whole():
                arrivals(place(t))
                for b in range(planes):
                    take_left(b, b, place(t))

            def fill():
                pl.when(t < aided)(alone)
                pl.when(t >= aided)(whole)
                multiply(t, planes * size, right_hi, right_lo)

            @pl.when(t == last)
            def _():
                terms_last()
                small(0)
            slot(t, last, fill, deliver)
            @pl.when(t == last)
            def _():
                small(1)
            return 0

        lax.fori_loop(0, chunks, step, 0)
        drain(last, deliver)
        for g in range(aided):
            give_copy(g).wait_recv()
            got_x[rows(g)] += got_x[rows(chunks + g)]
            out_copy(g, lead + g).start()
        for i in range(chunks):
            out_copy(0, i).wait()
        for j in range(4):
            aid_copy(first_b, j).wait_send()
            aid_copy(mid_b, j).wait_send()

    @pl.when(inner)
    def _():
        last = chunks + aided - 1
        keep = 1

        def deliver(t):
            @pl.when(t < early)
            def _():
                out_copy(t, t).start()
            @pl.when((t >= early) & (t < early + keep))
            def _():
                give_copy(t - early).start()
            @pl.when(t >= early + aided)
            def _():
                out_copy(t, t - aided).start()

        def take_aid():
            def stage(b, j, at):
                return pltpu.make_async_copy(aid_hbm.at[b, j], far_rows.at[at // 4, at % 4], rows_sem.at[at // 4, at % 4])

            for j in range(4):
                aid_copy(mid_b, j).wait_recv()
                stage(first_b, j, j).start()
                stage(mid_b, j, 4 + j).start()
            for j in range(4):
                stage(first_b, j, j).wait()
                keep_right(aid_hi, aid_lo, far_rows[0, j], j, first_b - low)
                aid_y_copy(other_b, j).wait_recv()
                stage(other_b, j, j).start()
            for j in range(4):
                stage(mid_b, j, 4 + j).wait()
                keep_right(aid_hi, aid_lo, far_rows[1, j], j, mid_b - low)
            for j in range(4):
                stage(other_b, j, j).wait()
                keep_right(aid_hi, aid_lo, far_rows[0, j], j, other_b - low)

        def step(t, _):
            def events(at):
                if at < first:
                    came_in(first + at - 1)
                    if at == 2:
                        came_far(first - 1)
                elif at == first:
                    came_in(chunks - 1)
                    take_aid()
                    came_out(first)
                elif at == first + 1:
                    came_out(first + 1)
                elif at == first + 2:
                    came_far(first)
                elif at == first + aided - 1:
                    came_far(first + 1)
                elif at == first + aided + 1:
                    came_out(first + 2)
                    came_out(first + 3)
                    came_far(first + 2)
                elif at < last - 1:
                    came_out(at - aided + 2)
                    came_far(at - aided + 1)
                else:
                    came_far(chunks - 1)
                    for g in range(keep, aided):
                        give_copy(g).start()

            for at in (*range(1, first + 3), *range(first + aided - 1, chunks + aided - 1)):
                if at != first + aided:
                    pl.when(t == at)(functools.partial(events, at))

            def fill():
                @pl.when((t >= early) & (t < early + aided))
                def _():
                    for at in range(planes - 1):
                        take_left(at, at + low, t - early + lead)
                    multiply(t, (planes - 1) * size, aid_hi, aid_lo)

                @pl.when((t < early) | (t >= early + aided))
                def _():
                    i = t - aided * lax.div(t, early + aided)
                    for b in range(planes):
                        take_left(b, b, i)
                    multiply(t, planes * size, right_hi, right_lo)

            slot(t, last, fill, deliver)
            @pl.when(t == first + aided)
            def _():
                terms_on()
            @pl.when(t == first + aided + 2)
            def _():
                terms_in()
                small(0)
            @pl.when(t == first + aided + 3)
            def _():
                small(1)
            return 0

        lax.fori_loop(0, chunks + aided, step, 0)
        drain(last, deliver)
        for i in range(chunks):
            out_copy(0, i).wait()
        for g in range(aided):
            give_copy(g).wait_send()
        for j in range(4):
            aid_y_copy(first_b, j).wait_send()

    small(4)

    pltpu.make_async_copy(app_ref, app_hbm, app_sem.at[0]).wait()
    fac_y.wait_send()
    t_core_copy.wait_send()
    t_x_copy.wait_send()
    for far in range(1, planes):
        sz_copy(far).wait_send()
    for b in range(planes):
        @pl.when(b != c)
        def _():
            line_copy(0, b, b).wait_send()
    for stage, mate in enumerate((core_mate, x_mate, y_mate)):
        s_copy(stage, mate).wait_send()
    for q in range(per_row):
        for j in range(4):
            y_copy(q, j).wait_send()

    def finish(i, _):
        for b in range(planes):
            for way in (0, 1):
                sends = (b <= c) if way == 0 else (b >= c)
                @pl.when(goes(way, i) & sends)
                def _():
                    @pl.when(b == c)
                    def _():
                        hop(way, b, i, own=True).wait_send()
                    @pl.when(b != c)
                    def _():
                        hop(way, b, i).wait_send()
        return 0

    lax.fori_loop(0, chunks, finish, 0)


def hand_over(sq_hbm, app_hbm, norm_hbm, sq_out, app_out, norm_out, sq_buf, app_buf, norm_buf, in_sem, out_sem):
    parts = in_sem.shape[0] - 2
    tall = sq_buf.shape[0] // parts
    places = [pl.ds(i * tall, tall) for i in range(parts)]
    moves = [(sq_hbm.at[at], sq_buf.at[at], sq_out.at[at]) for at in places]
    moves += [(app_hbm, app_buf, app_out), (norm_hbm, norm_buf, norm_out)]
    ins = [pltpu.make_async_copy(src, buf, in_sem.at[i]) for i, (src, buf, _) in enumerate(moves)]
    outs = [pltpu.make_async_copy(buf, dst, out_sem.at[i]) for i, (_, buf, dst) in enumerate(moves)]
    for copy in ins:
        copy.start()
    for taken, given in zip(ins, outs):
        taken.wait()
        given.start()
    for copy in outs:
        copy.wait()


def fused(planes, state_matrix, gram_factor):
    block_rows, block_cols = state_matrix.shape
    size = block_cols // 4
    tall = size // 2
    chunks = block_rows // tall
    aided = chunks // 4
    ring = 6
    factor_rows, half = gram_factor.shape
    rank = 2 * half
    piece = block_rows // (planes * 4)
    per_row = block_rows // block_cols
    f32, bf16 = jnp.float32, jnp.bfloat16
    dma = pltpu.SemaphoreType.DMA
    scratch = [
        pltpu.VMEM((planes, block_rows, size), f32),
        pltpu.VMEM((tall, planes * size), bf16),
        pltpu.VMEM((tall, planes * size), bf16),
        pltpu.VMEM((per_row, 4, size, size), f32),
        pltpu.VMEM((2, planes * size, 2 * size), bf16),
        pltpu.VMEM((2, planes * size, 2 * size), bf16),
        pltpu.VMEM((2, (planes - 1) * size, 2 * size), bf16),
        pltpu.VMEM((2, (planes - 1) * size, 2 * size), bf16),
        pltpu.VMEM((2, 2, 2, tall, size), f32),
        pltpu.VMEM((ring, 2, tall, size), f32),
        pltpu.VMEM(((chunks + aided) * tall, size), f32),
        pltpu.VMEM((factor_rows, rank), f32),
        pltpu.VMEM((factor_rows, rank), bf16),
        pltpu.VMEM((factor_rows, rank), bf16),
        pltpu.VMEM((planes, 2, 2, piece, rank), f32),
        pltpu.VMEM((planes, 2, piece, rank), f32),
        pltpu.VMEM((planes, piece, rank), f32),
        pltpu.VMEM((planes + 1, piece, rank), f32),
        pltpu.VMEM((4, 8, rank), f32),
        pltpu.VMEM((3, 8, rank), f32),
        pltpu.VMEM((planes, 8, rank), f32),
        pltpu.VMEM((piece, rank), f32),
        dma((1,)), dma((per_row, 4)), dma((chunks,)), dma((1,)), dma((1,)),
        dma((planes + 1, chunks)), dma((planes, chunks)),
        dma((per_row, 4)), dma((per_row, 4)),
        dma((chunks + aided,)), dma((chunks + aided,)), dma((chunks + aided,)), dma((chunks + aided,)),
        dma((6,)), dma((6,)), dma((planes,)), dma((planes + 1,)), dma((planes,)), dma((planes,)),
        dma((planes, 4)), dma((planes, 4)), dma((4,)), dma((4,)), dma((aided,)), dma((aided,)),
        pltpu.SemaphoreType.REGULAR,
    ]
    squared, appended, norm, _ = pl.pallas_call(
        functools.partial(kernel, planes, aided),
        out_shape=[
            jax.ShapeDtypeStruct((block_rows, size), f32),
            jax.ShapeDtypeStruct((piece, rank), f32),
            jax.ShapeDtypeStruct((1, rank), f32),
            jax.ShapeDtypeStruct((planes, 4, size, size), f32),
        ],
        in_specs=[pl.BlockSpec(memory_space=pl.ANY)] * 2,
        out_specs=[
            pl.BlockSpec(memory_space=pl.ANY),
            pl.BlockSpec(memory_space=pl.ANY),
            pl.BlockSpec(memory_space=pltpu.VMEM),
            pl.BlockSpec(memory_space=pl.ANY),
        ],
        scratch_shapes=scratch,
        compiler_params=pltpu.CompilerParams(collective_id=0, has_side_effects=True, vmem_limit_bytes=VMEM_BYTES),
    )(state_matrix, gram_factor)
    parts = 8
    results = (squared, appended, norm)
    squared, appended, norm = pl.pallas_call(
        hand_over,
        out_shape=[jax.ShapeDtypeStruct(r.shape, r.dtype) for r in results],
        in_specs=[pl.BlockSpec(memory_space=pl.ANY)] * 3,
        out_specs=[pl.BlockSpec(memory_space=pl.ANY)] * 3,
        scratch_shapes=[pltpu.VMEM(r.shape, r.dtype) for r in results] + [dma((parts + 2,)), dma((parts + 2,))],
    )(*results)
    return squared, appended, norm[0]


def product(left, right):
    return jnp.dot(left, right, preferred_element_type=jnp.float32, precision=lax.Precision.HIGH)


def halving_order(count):
    order = [0]
    step = 1
    while step < count:
        order = [2 * j for j in order] + [2 * j + 1 for j in order]
        step *= 2
    return order


def exchange(value, bit, count):
    return lax.ppermute(value, "depth", [(d, d ^ bit) for d in range(count)])


def body(state_matrix, gram_factor):
    row_count = lax.axis_size("row")
    col_count = lax.axis_size("col")
    depth_count = lax.axis_size("depth")
    row_index = lax.axis_index("row")
    col_index = lax.axis_index("col")
    depth_index = lax.axis_index("depth")
    block_rows, block_cols = state_matrix.shape
    slab = block_cols // depth_count
    blocks_per_row = block_rows // block_cols
    order = halving_order(depth_count)

    own_columns = lax.dynamic_slice_in_dim(state_matrix, depth_index * slab, slab, 1)
    edges = [block_rows * part // 16 for part in (0, 7, 13, 16)]
    lefts = [
        lax.all_gather(own_columns[low:high], "col", axis=1, tiled=True) for low, high in zip(edges, edges[1:])
    ]

    stacked = state_matrix.reshape(blocks_per_row, block_cols, block_cols)
    own_rows = lax.dynamic_slice_in_dim(stacked, depth_index * slab, slab, 1).reshape(
        blocks_per_row * slab, block_cols
    )
    own_rows = jnp.concatenate(
        [lax.dynamic_slice_in_dim(own_rows, (depth_index ^ j) * slab, slab, 1) for j in order], axis=1
    )

    def row_gather(value):
        pieces = [value]
        for s in range(1, row_count):
            pieces.append(lax.ppermute(value, "row", [(r, (r + s) % row_count) for r in range(row_count)]))
        ordered = []
        for r in range(row_count):
            piece = pieces[0]
            for s in range(1, row_count):
                piece = jnp.where(lax.rem(row_index + (row_count - r), row_count) == s, pieces[s], piece)
            ordered.append(piece)
        return ordered

    factor_block = jnp.concatenate(row_gather(gram_factor), axis=1)
    column_block = jnp.concatenate(row_gather(own_rows), axis=0)

    terms = product(own_columns, factor_block)
    piece_rows = block_rows // (col_count * depth_count)
    terms = terms.reshape(col_count, depth_count, piece_rows, terms.shape[1])
    held = jnp.concatenate(
        [lax.dynamic_slice_in_dim(terms, depth_index ^ j, 1, 1) for j in order], axis=1
    )
    bit, width = 1, depth_count
    while width > 1:
        width //= 2
        held = held[:, :width] + exchange(held[:, width:], bit, depth_count)
        bit *= 2
    held = held[:, 0]
    new_rows = lax.dynamic_index_in_dim(held, col_index, 0, keepdims=False)
    for s in range(1, col_count):
        part = lax.dynamic_index_in_dim(held, lax.rem(col_index + s, col_count), 0, keepdims=False)
        new_rows = new_rows + lax.ppermute(part, "col", [(c, (c + s) % col_count) for c in range(col_count)])
    new_sq = jnp.sum(new_rows * new_rows, axis=0)
    old_sq = jnp.sum(factor_block * factor_block, axis=0) * (1.0 / row_count)
    totals_new, totals_old = lax.psum((new_sq, old_sq), ("row", "col", "depth"))
    norm_ratio = jnp.sqrt(totals_new) / jnp.sqrt(totals_old + 1e-06)

    half = block_cols // 2
    outs = []
    for left in lefts:
        if outs:
            left, outs[-1], norm_ratio = lax.optimization_barrier((left, outs[-1], norm_ratio))
        if depth_count == 1:
            outs.append(product(left, column_block))
            continue
        sent = exchange(product(left, column_block[:, half:]), 1, depth_count)
        total = product(left, column_block[:, :half]) + sent
        bit, width = 2, half
        while width > slab:
            width //= 2
            total = total[:, :width] + exchange(total[:, width:], bit, depth_count)
            bit *= 2
        outs.append(total)
    squared = jnp.concatenate(outs, axis=0)
    return (squared, new_rows, norm_ratio)


def solution(mesh):
    in_specs = (P("row", "col"), P(("col", "depth"), "row"))
    out_specs = (P("row", ("col", "depth")), P(("row", "col", "depth"), None), P())

    def run(state_matrix, gram_factor):
        rows, cols = state_matrix.shape
        planes = mesh.shape["col"]
        whole_chunks = rows % cols == 0 and cols % (128 * 4) == 0 and gram_factor.shape[1] % 128 == 0
        paired = mesh.shape["row"] == 2 and mesh.shape["depth"] == 4 and planes == 4 and 2 * cols == rows
        if whole_chunks and paired:
            return fused(planes, state_matrix, gram_factor)
        return body(state_matrix, gram_factor)

    return jax.shard_map(run, mesh=mesh, in_specs=in_specs, out_specs=out_specs, check_vma=False)
```

```python
import functools

import jax
import jax.numpy as jnp
from jax import lax
from jax.experimental import pallas as pl
from jax.experimental.pallas import tpu as pltpu
from jax.sharding import PartitionSpec as P


MESH = pl.DeviceIdType.MESH
VMEM_BYTES = 66_900_000


def split(value):
    high = value.astype(jnp.bfloat16)
    return high, (value - high.astype(jnp.float32)).astype(jnp.bfloat16)


def dot(left, right):
    return jnp.dot(left, right, preferred_element_type=jnp.float32)


def kernel(
    planes, aided, a_hbm, z_hbm, sq_hbm, app_hbm, norm_ref, aid_hbm,
    left, left_hi, left_lo, far_rows, right_hi, right_lo, aid_hi, aid_lo, part, got_core, got_x,
    fac, fac_hi, fac_lo, terms, t_core, t_x, t_z, sums, s_got, s_z, app_ref,
    own_sem, rows_sem, out_sem, fac_own_sem, app_sem, z_send, z_recv, y_send, y_recv, core_send, core_recv,
    x_send, x_recv, small_send, small_recv, tz_send, tz_recv, sz_send, sz_recv,
    aid_send, aid_recv, aid_y_send, aid_y_recv, give_send, give_recv, credit,
):
    y, c, d = lax.axis_index("row"), lax.axis_index("col"), lax.axis_index("depth")
    x, k = lax.div(d, 2), lax.rem(d, 2)
    core_mate = {"depth": d + 1 - 2 * k}
    x_mate = {"depth": lax.rem(d + 2, 4)}
    y_mate = {"row": 1 - y}
    tall, size = part.shape[3:]
    chunks = left.shape[1] // tall
    lead = 1
    first = chunks // 2
    early = first
    ring = got_core.shape[0]
    lag = ring - 2
    per_row = a_hbm.shape[0] // a_hbm.shape[1]
    block = a_hbm.shape[1]
    inner = (c > 0) & (c < planes - 1)
    outer = jnp.logical_not(inner)
    own_cols = pl.ds(pl.multiple_of(d * size, size), size)
    low = 1 - lax.div(c, 2)
    minor = lax.rem(y + low, 2)
    aid_to = {"col": 3 - 3 * low}
    aid_from = {"col": 2 - low}
    near_b, mid_b, far_b = 2 - low, 1 + low, 3 * low
    first_b = far_b + (near_b - far_b) * minor
    other_b = near_b + (far_b - near_b) * minor

    def rows(i):
        return pl.ds(pl.multiple_of(i * tall, tall), tall)

    def remote(src, dst, send, recv, target):
        return pltpu.make_async_remote_copy(
            src_ref=src, dst_ref=dst, send_sem=send, recv_sem=recv, device_id=target, device_id_type=MESH
        )

    def hop(way, b, i, own=False):
        src = a_hbm.at[rows(i), own_cols] if own else left.at[b, rows(i)]
        target = {"col": c + 1 - 2 * way}
        line = planes if own and way == 1 else b
        return remote(src, left.at[b, rows(i)], z_send.at[line, i], z_recv.at[b, i], target)

    def shared(i):
        return (i < lead) | (i >= lead + aided)

    def goes(way, i):
        if way == 0:
            return (c < planes - 2) | ((c == planes - 2) & shared(i))
        return (c > 1) | ((c == 1) & shared(i))

    def send_own(i, ways=(0, 1)):
        for way in ways:
            @pl.when(goes(way, i))
            def _():
                hop(way, c, i, own=True).start()

    def to_center(i):
        pl.when(low == 1)(lambda: send_own(i, (0,)))
        pl.when(low == 0)(lambda: send_own(i, (1,)))

    def to_end(i):
        pl.when(low == 1)(lambda: send_own(i, (1,)))
        pl.when(low == 0)(lambda: send_own(i, (0,)))

    def arrivals(i):
        for b in range(planes):
            @pl.when(b != c)
            def _():
                hop(0, b, i).wait_recv()

    def pass_on(way, b, i):
        hop(way, b, i).wait_recv()
        @pl.when(goes(way, i))
        def _():
            hop(way, b, i).start()

    def came_out(i):
        pl.when(low == 1)(lambda: pass_on(0, 0, i))
        pl.when(low == 0)(lambda: pass_on(1, planes - 1, i))

    def came_in(i):
        pl.when(low == 1)(lambda: pass_on(1, 2, i))
        pl.when(low == 0)(lambda: pass_on(0, 1, i))

    def came_far(i):
        pl.when(low == 1)(lambda: pass_on(1, planes - 1, i))
        pl.when(low == 0)(lambda: pass_on(0, 0, i))

    own_copy = pltpu.make_async_copy(a_hbm.at[:, own_cols], left.at[c], own_sem.at[0])

    def right_rows(q, j):
        return a_hbm.at[pl.ds(pl.multiple_of(q * block + d * size, size), size), pl.ds(j * size, size)]

    def near_place(q, j):
        return got_x.at[pl.ds((q * 4 + j) * size, size)]

    def near_copy(q, j):
        return pltpu.make_async_copy(right_rows(q, j), near_place(q, j), rows_sem.at[q, j])

    def y_copy(q, j):
        return remote(right_rows(q, j), far_rows.at[q, j], y_send.at[q, j], y_recv.at[q, j], y_mate)

    def aid_copy(b, j, from_far=False):
        q = low if b is first_b else 1 - low
        src = far_rows.at[q, j] if from_far else right_rows(q, j)
        return remote(src, aid_hbm.at[b, j], aid_send.at[b, j], aid_recv.at[b, j], aid_from)

    def aid_y_copy(b, j):
        return remote(aid_hbm.at[b, j], aid_hbm.at[b, j], aid_y_send.at[j], aid_y_recv.at[j], y_mate)

    own_copy.start()
    for q in range(per_row):
        for j in range(4):
            near_copy(q, j).start()
    barrier = pltpu.get_barrier_semaphore()
    mates = [core_mate, x_mate, y_mate] + [{"col": lax.rem(c + far, planes)} for far in range(1, planes)]
    for mate in mates:
        pl.semaphore_signal(barrier, inc=1, device_id=mate, device_id_type=MESH)
    pl.semaphore_wait(barrier, len(mates))
    half = z_hbm.shape[1]
    lanes = pl.ds(pl.multiple_of(y * half, half), half)
    fac_own = pltpu.make_async_copy(z_hbm, fac.at[:, lanes], fac_own_sem.at[0])
    fac_y = remote(z_hbm, fac.at[:, lanes], small_send.at[0], small_recv.at[0], y_mate)
    fac_y.start()
    fac_own.start()
    @pl.when(inner)
    def _():
        for i in range(first // 2):
            to_center(i)
        for i in range(chunks):
            if not lead <= i < lead + aided:
                to_end(i)
    for j in range(4):
        for q in range(per_row):
            y_copy(q, j).start()
    @pl.when(outer)
    def _():
        for i in range(first):
            send_own(i)
        for j in range(4):
            aid_copy(first_b, j).start()

    def keep_right(high_ref, low_ref, value, j, at):
        high, rest = split(value)
        at = pl.ds(pl.multiple_of(at * size, size), size)
        high_ref[j // 2, at, j % 2 * size : (j % 2 + 1) * size] = high
        low_ref[j // 2, at, j % 2 * size : (j % 2 + 1) * size] = rest

    own_copy.wait()
    fac_own.wait()
    fac_y.wait_recv()
    fac_hi[...], fac_lo[...] = split(fac[...])
    piece = terms.shape[3]

    def term(i, _):
        high, rest = split(left[c, pl.ds(pl.multiple_of(i * size, size), size)])
        value = dot(high, fac_hi[...]) + dot(high, fac_lo[...]) + dot(rest, fac_hi[...])
        for half_k in (0, 1):
            terms[lax.div(i, 2), lax.rem(i, 2), half_k] = value[half_k * piece : (half_k + 1) * piece]
        return 0

    lax.fori_loop(0, left.shape[1] // size, term, 0)
    for q in range(per_row):
        for j in range(4):
            near_copy(q, j).wait()
            keep_right(right_hi, right_lo, near_place(q, j)[...], j, y * per_row + q)
    t_core_copy = remote(terms.at[:, :, 1 - k], t_core, small_send.at[1], small_recv.at[1], core_mate)
    t_core_copy.start()
    t_core_copy.wait_recv()
    for b in range(planes):
        t_core[b, 0] += terms[b, 0, k]
        t_core[b, 1] += terms[b, 1, k]
    @pl.when(inner)
    def _():
        for i in (0, 1):
            came_out(i)
            came_in(i)
            to_center(i + first // 2)
    t_x_copy = remote(t_core.at[:, 1 - x], t_x, small_send.at[2], small_recv.at[2], x_mate)
    t_x_copy.start()
    t_x_copy.wait_recv()
    for b in range(planes):
        t_x[b] += t_core[b, x]
    @pl.when(inner)
    def _():
        came_far(0)

    def line_copy(way, b, at, src=None):
        target = {"col": c + 1 - 2 * way}
        src = t_z.at[at] if src is None else src
        return remote(src, t_z.at[at], tz_send.at[b], tz_recv.at[at], target)

    def line_send(way, b, own=False):
        src = t_x.at[b] if own else t_z.at[b]
        if way == 0:
            return line_copy(0, b, b, src)
        mine = b == planes - 2 if own else b < 2
        return line_copy(1, b, planes if mine else b, src)

    def line_got(at):
        line_copy(0, 0, at).wait_recv()

    def terms_off():
        @pl.when(low == 1)
        def _():
            for b in range(1, planes):
                line_send(0, b, own=True).start()
        @pl.when(low == 0)
        def _():
            for b in range(planes - 1):
                line_send(1, b, own=True).start()

    def terms_on():
        @pl.when(low == 1)
        def _():
            for b in (1, 2, 3):
                line_got(b)
            for b in (2, 3):
                t_z[b] += t_x[b]
                line_send(0, b).start()
        @pl.when(low == 0)
        def _():
            for at in (0, 1, planes):
                line_got(at)
            for b in (0, 1):
                t_z[b] += t_x[b]
            line_copy(1, 0, 0).start()
            line_send(1, 1).start()

    def terms_in():
        @pl.when(low == 1)
        def _():
            line_got(0)
            line_got(planes)
            t_z[0] += t_x[0]
            line_send(1, 0).start()
            app_ref[...] = t_x[1] + t_z[1] + t_z[planes]
        @pl.when(low == 0)
        def _():
            line_got(2)
            line_got(3)
            t_z[3] += t_x[3]
            line_send(0, 3).start()
            app_ref[...] = t_x[2] + t_z[2] + t_z[planes]

    def terms_last():
        @pl.when(low == 1)
        def _():
            line_got(planes)
            app_ref[...] = t_x[0] + t_z[planes]
        @pl.when(low == 0)
        def _():
            line_got(planes - 1)
            app_ref[...] = t_x[planes - 1] + t_z[planes - 1]

    @pl.when(inner)
    def _():
        for i in range(2, first):
            came_out(i)
            came_in(i)
            to_center(i + first // 2)
            came_far(i - 1)
        for i in range(first + first // 2, chunks):
            to_center(i)

    for j in range(4):
        for q in range(per_row):
            y_copy(q, j).wait_recv()
            keep_right(right_hi, right_lo, far_rows[q, j], j, (1 - y) * per_row + q)
        @pl.when(outer)
        def _():
            for piece_j in ((), (), (0, 1, 2), (3,))[j]:
                @pl.when(minor == 0)
                def _():
                    aid_copy(mid_b, piece_j).start()
                @pl.when(minor == 1)
                def _():
                    aid_copy(mid_b, piece_j, from_far=True).start()
    @pl.when(outer)
    def _():
        for i in range(first, first + 2):
            send_own(i)
        terms_off()
        for i in range(first + 2, chunks):
            send_own(i)
    @pl.when(inner)
    def _():
        for j in range(4):
            aid_copy(first_b, j).wait_recv()
            aid_y_copy(first_b, j).start()

    def s_copy(stage, target):
        return remote(sums.at[stage], s_got.at[stage], small_send.at[3 + stage], small_recv.at[3 + stage], target)

    def sz_copy(far):
        b = lax.rem(c + far, planes)
        return remote(sums.at[3], s_z.at[c], sz_send.at[far - 1], sz_recv.at[c], {"col": b})

    def sz_arrival(b):
        return remote(sums.at[3], s_z.at[b], sz_send.at[0], sz_recv.at[b], {"col": b})

    def small(step):
        if step == 0:
            total = app_ref[...]
            pltpu.make_async_copy(app_ref, app_hbm, app_sem.at[0]).start()
            new = jnp.sum(total * total, axis=0, keepdims=True)
            old = jnp.sum(fac[...] * fac[...], axis=0, keepdims=True) * 0.5
            sums[0, 0:1] = new
            sums[0, 1:2] = old
            s_copy(0, core_mate).start()
        elif step == 1:
            s_copy(0, core_mate).wait_recv()
            sums[1, 0:2] = sums[0, 0:2] + s_got[0, 0:2]
            s_copy(1, x_mate).start()
        elif step == 2:
            s_copy(1, x_mate).wait_recv()
            sums[2, 0:2] = sums[1, 0:2] + s_got[1, 0:2]
            s_copy(2, y_mate).start()
        elif step == 3:
            s_copy(2, y_mate).wait_recv()
            sums[3, 0:2] = sums[2, 0:2] + s_got[2, 0:2]
            for far in range(1, planes):
                sz_copy(far).start()
        elif step == 4:
            for b in range(planes):
                @pl.when(b != c)
                def _():
                    sz_arrival(b).wait_recv()
            s_z[c, 0:2] = sums[3, 0:2]
            both = s_z[0, 0:2]
            for b in range(1, planes):
                both = both + s_z[b, 0:2]
            norm_ref[...] = jnp.sqrt(both[0:1]) / jnp.sqrt(both[1:2] + 1e-06)

    def core_copy(t):
        return remote(
            part.at[lax.rem(t, 2), :, 1 - k], got_core.at[lax.rem(t, ring)], core_send.at[t], core_recv.at[t], core_mate
        )

    def x_copy(t):
        return remote(got_core.at[lax.rem(t, ring), 1 - x], got_x.at[rows(t)], x_send.at[t], x_recv.at[t], x_mate)

    def out_copy(t, i):
        return pltpu.make_async_copy(got_x.at[rows(t)], sq_hbm.at[rows(i)], out_sem.at[i])

    def give_copy(g):
        return remote(got_x.at[rows(early + g)], got_x.at[rows(chunks + g)], give_send.at[g], give_recv.at[g], aid_to)

    def take_left(at, b, i):
        high, rest = split(left[b, rows(i)])
        left_hi[:, at * size : (at + 1) * size] = high
        left_lo[:, at * size : (at + 1) * size] = rest

    def multiply(t, width, high_ref, low_ref):
        def side(s, _):
            high, rest = left_hi[:, :width], left_lo[:, :width]
            value = dot(high, high_ref[s]) + dot(high, low_ref[s]) + dot(rest, high_ref[s])
            part[lax.rem(t, 2), s, 0] = value[:, :size]
            part[lax.rem(t, 2), s, 1] = value[:, size:]
            return 0

        lax.fori_loop(0, 2, side, 0)

    def after_core(t):
        core_copy(t).wait_recv()
        at = lax.rem(t, ring)
        got_core[at, 1 - x] += part[lax.rem(t, 2), 1 - x, k]
        got_core[at, x] += part[lax.rem(t, 2), x, k]
        x_copy(t).start()

    def after_x(t, last):
        x_copy(t).wait_recv()
        got_x[rows(t)] += got_core[lax.rem(t, ring), x]
        x_copy(t).wait_send()
        @pl.when(t + ring <= last)
        def _():
            pl.semaphore_signal(credit, inc=1, device_id=core_mate, device_id_type=MESH)

    def slot(t, last, fill, deliver):
        @pl.when(t >= 2)
        def _():
            core_copy(t - 2).wait_send()
        fill()
        @pl.when(t >= 1)
        def _():
            after_core(t - 1)
        @pl.when(t >= ring)
        def _():
            pl.semaphore_wait(credit, 1)
        core_copy(t).start()
        @pl.when(t >= lag)
        def _():
            after_x(t - lag, last)
            deliver(t - lag)

    def drain(last, deliver):
        after_core(last)
        for back in range(lag - 1, 0, -1):
            after_x(last - back, last)
            deliver(last - back)
        small(2)
        small(3)
        after_x(last, last)
        deliver(last)
        core_copy(last - 1).wait_send()
        core_copy(last).wait_send()

    @pl.when(outer)
    def _():
        last = chunks - 1

        def place(t):
            return t - aided + aided * lax.div(t + chunks - lead - aided, chunks)

        def deliver(t):
            @pl.when(t >= aided)
            def _():
                out_copy(t, place(t)).start()

        def step(t, _):
            def alone():
                for b in range(planes):
                    @pl.when(b == c)
                    def _():
                        take_left(b, b, lead + t)
                    @pl.when(b != c)
                    def _():
                        left_hi[:, b * size : (b + 1) * size] = jnp.zeros((tall, size), jnp.bfloat16)
                        left_lo[:, b * size : (b + 1) * size] = jnp.zeros((tall, size), jnp.bfloat16)

            def whole():
                arrivals(place(t))
                for b in range(planes):
                    take_left(b, b, place(t))

            def fill():
                pl.when(t < aided)(alone)
                pl.when(t >= aided)(whole)
                multiply(t, planes * size, right_hi, right_lo)

            @pl.when(t == last)
            def _():
                terms_last()
                small(0)
            slot(t, last, fill, deliver)
            @pl.when(t == last)
            def _():
                small(1)
            return 0

        lax.fori_loop(0, chunks, step, 0)
        drain(last, deliver)
        for g in range(aided):
            give_copy(g).wait_recv()
            got_x[rows(g)] += got_x[rows(chunks + g)]
            out_copy(g, lead + g).start()
        for i in range(chunks):
            out_copy(0, i).wait()
        for j in range(4):
            aid_copy(first_b, j).wait_send()
            aid_copy(mid_b, j).wait_send()

    @pl.when(inner)
    def _():
        last = chunks + aided - 1
        keep = 1

        def deliver(t):
            @pl.when(t < early)
            def _():
                out_copy(t, t).start()
            @pl.when((t >= early) & (t < early + keep))
            def _():
                give_copy(t - early).start()
            @pl.when(t >= early + aided)
            def _():
                out_copy(t, t - aided).start()

        def take_aid():
            def stage(b, j, at):
                return pltpu.make_async_copy(aid_hbm.at[b, j], far_rows.at[at // 4, at % 4], rows_sem.at[at // 4, at % 4])

            for j in range(4):
                aid_copy(mid_b, j).wait_recv()
                stage(first_b, j, j).start()
                stage(mid_b, j, 4 + j).start()
            for j in range(4):
                stage(first_b, j, j).wait()
                keep_right(aid_hi, aid_lo, far_rows[0, j], j, first_b - low)
                aid_y_copy(other_b, j).wait_recv()
                stage(other_b, j, j).start()
            for j in range(4):
                stage(mid_b, j, 4 + j).wait()
                keep_right(aid_hi, aid_lo, far_rows[1, j], j, mid_b - low)
            for j in range(4):
                stage(other_b, j, j).wait()
                keep_right(aid_hi, aid_lo, far_rows[0, j], j, other_b - low)

        def step(t, _):
            def events(at):
                if at < first:
                    came_in(first + at - 1)
                    if at == 2:
                        came_far(first - 1)
                elif at == first:
                    came_in(chunks - 1)
                    take_aid()
                    came_out(first)
                elif at == first + 1:
                    came_out(first + 1)
                elif at == first + 2:
                    came_far(first)
                elif at == first + aided - 1:
                    came_far(first + 1)
                elif at == first + aided + 1:
                    came_out(first + 2)
                    came_out(first + 3)
                    came_far(first + 2)
                elif at < last - 1:
                    came_out(at - aided + 2)
                    came_far(at - aided + 1)
                else:
                    came_far(chunks - 1)
                    for g in range(keep, aided):
                        give_copy(g).start()

            for at in (*range(1, first + 3), *range(first + aided - 1, chunks + aided - 1)):
                if at != first + aided:
                    pl.when(t == at)(functools.partial(events, at))

            def fill():
                @pl.when((t >= early) & (t < early + aided))
                def _():
                    for at in range(planes - 1):
                        take_left(at, at + low, t - early + lead)
                    multiply(t, (planes - 1) * size, aid_hi, aid_lo)

                @pl.when((t < early) | (t >= early + aided))
                def _():
                    i = t - aided * lax.div(t, early + aided)
                    for b in range(planes):
                        take_left(b, b, i)
                    multiply(t, planes * size, right_hi, right_lo)

            slot(t, last, fill, deliver)
            @pl.when(t == first + aided)
            def _():
                terms_on()
            @pl.when(t == first + aided + 1)
            def _():
                terms_in()
                small(0)
            @pl.when(t == first + aided + 2)
            def _():
                small(1)
            return 0

        lax.fori_loop(0, chunks + aided, step, 0)
        drain(last, deliver)
        for i in range(chunks):
            out_copy(0, i).wait()
        for g in range(aided):
            give_copy(g).wait_send()
        for j in range(4):
            aid_y_copy(first_b, j).wait_send()

    small(4)

    pltpu.make_async_copy(app_ref, app_hbm, app_sem.at[0]).wait()
    fac_y.wait_send()
    t_core_copy.wait_send()
    t_x_copy.wait_send()
    for far in range(1, planes):
        sz_copy(far).wait_send()
    for b in range(planes):
        @pl.when(b != c)
        def _():
            line_copy(0, b, b).wait_send()
    for stage, mate in enumerate((core_mate, x_mate, y_mate)):
        s_copy(stage, mate).wait_send()
    for q in range(per_row):
        for j in range(4):
            y_copy(q, j).wait_send()

    def finish(i, _):
        for b in range(planes):
            for way in (0, 1):
                sends = (b <= c) if way == 0 else (b >= c)
                @pl.when(goes(way, i) & sends)
                def _():
                    @pl.when(b == c)
                    def _():
                        hop(way, b, i, own=True).wait_send()
                    @pl.when(b != c)
                    def _():
                        hop(way, b, i).wait_send()
        return 0

    lax.fori_loop(0, chunks, finish, 0)


def hand_over(sq_hbm, app_hbm, norm_hbm, sq_out, app_out, norm_out, sq_buf, app_buf, norm_buf, in_sem, out_sem):
    parts = in_sem.shape[0] - 2
    tall = sq_buf.shape[0] // parts
    places = [pl.ds(i * tall, tall) for i in range(parts)]
    moves = [(sq_hbm.at[at], sq_buf.at[at], sq_out.at[at]) for at in places]
    moves += [(app_hbm, app_buf, app_out), (norm_hbm, norm_buf, norm_out)]
    ins = [pltpu.make_async_copy(src, buf, in_sem.at[i]) for i, (src, buf, _) in enumerate(moves)]
    outs = [pltpu.make_async_copy(buf, dst, out_sem.at[i]) for i, (_, buf, dst) in enumerate(moves)]
    for copy in ins:
        copy.start()
    for taken, given in zip(ins, outs):
        taken.wait()
        given.start()
    for copy in outs:
        copy.wait()


def fused(planes, state_matrix, gram_factor):
    block_rows, block_cols = state_matrix.shape
    size = block_cols // 4
    tall = size // 2
    chunks = block_rows // tall
    aided = chunks // 4
    ring = 5
    factor_rows, half = gram_factor.shape
    rank = 2 * half
    piece = block_rows // (planes * 4)
    per_row = block_rows // block_cols
    f32, bf16 = jnp.float32, jnp.bfloat16
    dma = pltpu.SemaphoreType.DMA
    scratch = [
        pltpu.VMEM((planes, block_rows, size), f32),
        pltpu.VMEM((tall, planes * size), bf16),
        pltpu.VMEM((tall, planes * size), bf16),
        pltpu.VMEM((per_row, 4, size, size), f32),
        pltpu.VMEM((2, planes * size, 2 * size), bf16),
        pltpu.VMEM((2, planes * size, 2 * size), bf16),
        pltpu.VMEM((2, (planes - 1) * size, 2 * size), bf16),
        pltpu.VMEM((2, (planes - 1) * size, 2 * size), bf16),
        pltpu.VMEM((2, 2, 2, tall, size), f32),
        pltpu.VMEM((ring, 2, tall, size), f32),
        pltpu.VMEM(((chunks + aided) * tall, size), f32),
        pltpu.VMEM((factor_rows, rank), f32),
        pltpu.VMEM((factor_rows, rank), bf16),
        pltpu.VMEM((factor_rows, rank), bf16),
        pltpu.VMEM((planes, 2, 2, piece, rank), f32),
        pltpu.VMEM((planes, 2, piece, rank), f32),
        pltpu.VMEM((planes, piece, rank), f32),
        pltpu.VMEM((planes + 1, piece, rank), f32),
        pltpu.VMEM((4, 8, rank), f32),
        pltpu.VMEM((3, 8, rank), f32),
        pltpu.VMEM((planes, 8, rank), f32),
        pltpu.VMEM((piece, rank), f32),
        dma((1,)), dma((per_row, 4)), dma((chunks,)), dma((1,)), dma((1,)),
        dma((planes + 1, chunks)), dma((planes, chunks)),
        dma((per_row, 4)), dma((per_row, 4)),
        dma((chunks + aided,)), dma((chunks + aided,)), dma((chunks + aided,)), dma((chunks + aided,)),
        dma((6,)), dma((6,)), dma((planes,)), dma((planes + 1,)), dma((planes,)), dma((planes,)),
        dma((planes, 4)), dma((planes, 4)), dma((4,)), dma((4,)), dma((aided,)), dma((aided,)),
        pltpu.SemaphoreType.REGULAR,
    ]
    squared, appended, norm, _ = pl.pallas_call(
        functools.partial(kernel, planes, aided),
        out_shape=[
            jax.ShapeDtypeStruct((block_rows, size), f32),
            jax.ShapeDtypeStruct((piece, rank), f32),
            jax.ShapeDtypeStruct((1, rank), f32),
            jax.ShapeDtypeStruct((planes, 4, size, size), f32),
        ],
        in_specs=[pl.BlockSpec(memory_space=pl.ANY)] * 2,
        out_specs=[
            pl.BlockSpec(memory_space=pl.ANY),
            pl.BlockSpec(memory_space=pl.ANY),
            pl.BlockSpec(memory_space=pltpu.VMEM),
            pl.BlockSpec(memory_space=pl.ANY),
        ],
        scratch_shapes=scratch,
        compiler_params=pltpu.CompilerParams(collective_id=0, has_side_effects=True, vmem_limit_bytes=VMEM_BYTES),
    )(state_matrix, gram_factor)
    parts = 4
    results = (squared, appended, norm)
    squared, appended, norm = pl.pallas_call(
        hand_over,
        out_shape=[jax.ShapeDtypeStruct(r.shape, r.dtype) for r in results],
        in_specs=[pl.BlockSpec(memory_space=pl.ANY)] * 3,
        out_specs=[pl.BlockSpec(memory_space=pl.ANY)] * 3,
        scratch_shapes=[pltpu.VMEM(r.shape, r.dtype) for r in results] + [dma((parts + 2,)), dma((parts + 2,))],
    )(*results)
    return squared, appended, norm[0]


def product(left, right):
    return jnp.dot(left, right, preferred_element_type=jnp.float32, precision=lax.Precision.HIGH)


def halving_order(count):
    order = [0]
    step = 1
    while step < count:
        order = [2 * j for j in order] + [2 * j + 1 for j in order]
        step *= 2
    return order


def exchange(value, bit, count):
    return lax.ppermute(value, "depth", [(d, d ^ bit) for d in range(count)])


def body(state_matrix, gram_factor):
    row_count = lax.axis_size("row")
    col_count = lax.axis_size("col")
    depth_count = lax.axis_size("depth")
    row_index = lax.axis_index("row")
    col_index = lax.axis_index("col")
    depth_index = lax.axis_index("depth")
    block_rows, block_cols = state_matrix.shape
    slab = block_cols // depth_count
    blocks_per_row = block_rows // block_cols
    order = halving_order(depth_count)

    own_columns = lax.dynamic_slice_in_dim(state_matrix, depth_index * slab, slab, 1)
    edges = [block_rows * part // 16 for part in (0, 7, 13, 16)]
    lefts = [
        lax.all_gather(own_columns[low:high], "col", axis=1, tiled=True) for low, high in zip(edges, edges[1:])
    ]

    stacked = state_matrix.reshape(blocks_per_row, block_cols, block_cols)
    own_rows = lax.dynamic_slice_in_dim(stacked, depth_index * slab, slab, 1).reshape(
        blocks_per_row * slab, block_cols
    )
    own_rows = jnp.concatenate(
        [lax.dynamic_slice_in_dim(own_rows, (depth_index ^ j) * slab, slab, 1) for j in order], axis=1
    )

    def row_gather(value):
        pieces = [value]
        for s in range(1, row_count):
            pieces.append(lax.ppermute(value, "row", [(r, (r + s) % row_count) for r in range(row_count)]))
        ordered = []
        for r in range(row_count):
            piece = pieces[0]
            for s in range(1, row_count):
                piece = jnp.where(lax.rem(row_index + (row_count - r), row_count) == s, pieces[s], piece)
            ordered.append(piece)
        return ordered

    factor_block = jnp.concatenate(row_gather(gram_factor), axis=1)
    column_block = jnp.concatenate(row_gather(own_rows), axis=0)

    terms = product(own_columns, factor_block)
    piece_rows = block_rows // (col_count * depth_count)
    terms = terms.reshape(col_count, depth_count, piece_rows, terms.shape[1])
    held = jnp.concatenate(
        [lax.dynamic_slice_in_dim(terms, depth_index ^ j, 1, 1) for j in order], axis=1
    )
    bit, width = 1, depth_count
    while width > 1:
        width //= 2
        held = held[:, :width] + exchange(held[:, width:], bit, depth_count)
        bit *= 2
    held = held[:, 0]
    new_rows = lax.dynamic_index_in_dim(held, col_index, 0, keepdims=False)
    for s in range(1, col_count):
        part = lax.dynamic_index_in_dim(held, lax.rem(col_index + s, col_count), 0, keepdims=False)
        new_rows = new_rows + lax.ppermute(part, "col", [(c, (c + s) % col_count) for c in range(col_count)])
    new_sq = jnp.sum(new_rows * new_rows, axis=0)
    old_sq = jnp.sum(factor_block * factor_block, axis=0) * (1.0 / row_count)
    totals_new, totals_old = lax.psum((new_sq, old_sq), ("row", "col", "depth"))
    norm_ratio = jnp.sqrt(totals_new) / jnp.sqrt(totals_old + 1e-06)

    half = block_cols // 2
    outs = []
    for left in lefts:
        if outs:
            left, outs[-1], norm_ratio = lax.optimization_barrier((left, outs[-1], norm_ratio))
        if depth_count == 1:
            outs.append(product(left, column_block))
            continue
        sent = exchange(product(left, column_block[:, half:]), 1, depth_count)
        total = product(left, column_block[:, :half]) + sent
        bit, width = 2, half
        while width > slab:
            width //= 2
            total = total[:, :width] + exchange(total[:, width:], bit, depth_count)
            bit *= 2
        outs.append(total)
    squared = jnp.concatenate(outs, axis=0)
    return (squared, new_rows, norm_ratio)


def solution(mesh):
    in_specs = (P("row", "col"), P(("col", "depth"), "row"))
    out_specs = (P("row", ("col", "depth")), P(("row", "col", "depth"), None), P())

    def run(state_matrix, gram_factor):
        rows, cols = state_matrix.shape
        planes = mesh.shape["col"]
        whole_chunks = rows % cols == 0 and cols % (128 * 4) == 0 and gram_factor.shape[1] % 128 == 0
        paired = mesh.shape["row"] == 2 and mesh.shape["depth"] == 4 and planes == 4 and 2 * cols == rows
        if whole_chunks and paired:
            return fused(planes, state_matrix, gram_factor)
        return body(state_matrix, gram_factor)

    return jax.shard_map(run, mesh=mesh, in_specs=in_specs, out_specs=out_specs, check_vma=False)
```
